32 devices in a mesh: gx: 4 (over y, x), gy: 4 (over z), ma: 2 (over core).
Axes of the slice: x: 2, y: 2, z: 4, core: 2. Of those that a mesh axis runs over, the one named last changes fastest.
Arguments:
- alpha_fields: bfloat16 [80, 2, 512, 512], P('ma', None, 'gy', 'gx'), may hold values from -6 to 6
- member_perts: bfloat16 [80, 2, 512, 512], P('ma', None, 'gy', 'gx'), may hold values from -0.625 to 0.625
- band_widths: int32 [2], replicated, may hold values from 2 to 8
- lat_index: int32 [1024], P('gy'), may hold values from 0 to 510, as said below
- lat_weight: float32 [1024], P('gy'), may hold values from 0 to 1
- lon_index: int32 [1024], P('gx'), may hold values from 0 to 511, as said below
- lon_weight: float32 [1024], P('gx'), may hold values from 0 to 1
- innovation: float32 [2, 1024, 1024], P(None, 'gy', 'gx'), may hold values from -6 to 6
- obs_weight: float32 [2, 1024, 1024], P(None, 'gy', 'gx'), may hold values from 0.1 to 1
Outputs:
- increment: float32 [2, 1024, 1024], P(None, 'gy', 'gx')
- gradient: float32 [80, 2, 512, 512], P('ma', None, 'gy', 'gx')
The draws below stay inside these ranges and needn't reach their ends.
Inputs may be any that keep to these rules, and one draw needn't show every extreme that they name: lat_index[p] is p // 2 - 1 or p // 2, clamped to 0 .. 510. lon_index[q] is q // 2 - 1 or q // 2, taken modulo 512.
All inputs are finite; a program needn't handle non-finite values.
Results may differ from the reference program's by a relative error of at most 0.0003.
Values may be sent and summed in bfloat16 or wider, within the bound.
No kernel may reach another device: no remote copies, remote signals or barrier semaphores. Data moves between devices by JAX's collectives and lax.ppermute only.
A program may use at most 128 MiB of HBM per device.

```python
import math
import jax
import jax.numpy as jnp
from jax import lax

MEM = 80
LEV = 2
HB = 8
NCLAT = 512
NCLON = 512
NFLAT = 1024
NFLON = 1024


def draw_lat_index(key, part):
    position = jnp.arange(NFLAT, dtype=jnp.int32)
    backward = jax.random.randint(key, (NFLAT,), 0, 2, dtype=jnp.int32)
    return jnp.clip(position // 2 - backward, 0, NCLAT - 2).astype(jnp.int32)


def draw_lon_index(key, part):
    position = jnp.arange(NFLON, dtype=jnp.int32)
    backward = jax.random.randint(key, (NFLON,), 0, 2, dtype=jnp.int32)
    return jnp.remainder(position // 2 - backward, NCLON).astype(jnp.int32)


def steps_of(own_key, dims, cuts, smallest, top_value):
    def one(dim, shards_of):
        heights = jax.random.uniform(jax.random.fold_in(jax.random.fold_in(own_key, 6), dim), (shards_of,), jnp.float32, smallest / len(cuts), top_value / len(cuts))
        return jnp.repeat(jnp.exp(heights), dims[dim] // shards_of).reshape((-1,) + (1,) * (len(dims) - dim - 1))

    gain = one(*cuts[0])
    for cut in cuts[1:]:
        gain = gain * one(*cut)
    return gain


def normal_values(rng, extent, width, limit, shards=(), kind=jnp.bfloat16):
    entries = width * jax.random.normal(rng, extent, jnp.float32)
    if shards:
        entries = entries * steps_of(rng, extent, shards, -0.22, 0.18)
    return jnp.clip(entries, -limit, limit).astype(kind)


def setup_inputs(seed: int = 0) -> dict:
    splits = jax.random.split(jax.random.key(seed), 10)
    return {
        "alpha_fields": normal_values(splits[0], (MEM, LEV, NCLAT, NCLON), 1.0, 6.0, ((0, 2), (2, 4), (3, 4))),
        "member_perts": normal_values(splits[1], (MEM, LEV, NCLAT, NCLON), MEM ** -0.5, 0.625, ((0, 2), (2, 4), (3, 4))),
        "band_widths": jax.random.randint(splits[2], (LEV,), 2, HB + 1).astype(jnp.int32),
        "lat_index": draw_lat_index(jax.random.fold_in(splits[9], 71), 0),
        "lat_weight": jnp.clip(1.0 * jax.random.uniform(splits[4], (NFLAT,), jnp.float32) ** steps_of(splits[4], (NFLAT,), ((0, 4),), -0.2, 0.2), 0.0, 1.0),
        "lon_index": draw_lon_index(jax.random.fold_in(splits[9], 71), 0),
        "lon_weight": jnp.clip(1.0 * jax.random.uniform(splits[6], (NFLON,), jnp.float32) ** steps_of(splits[6], (NFLON,), ((0, 4),), -0.2, 0.2), 0.0, 1.0),
        "innovation": normal_values(splits[7], (LEV, NFLAT, NFLON), 1.0, 6.0, ((1, 4), (2, 4)), jnp.float32),
        "obs_weight": jnp.clip(jnp.exp(math.log(1.0) - 2.3025851 * jax.random.uniform(splits[8], (LEV, NFLAT, NFLON), jnp.float32) ** steps_of(splits[8], (LEV, NFLAT, NFLON), ((1, 4), (2, 4)), -0.2, 0.2)), 0.1, 1.0),
    }


def tap_table(band_widths):
    tap_offsets = jnp.arange(-HB, HB + 1).astype(jnp.float32)
    spread = band_widths.astype(jnp.float32)[:, None]
    shapes = jnp.exp(-tap_offsets[None, :] ** 2 / (2.0 * spread * spread))
    return shapes / jnp.sqrt(lax.optimization_barrier(jnp.sum(shapes * shapes, axis=1, keepdims=True)))

def localize(source, filter_taps):
    along_lon = jnp.zeros_like(source)
    for tap_number in range(2 * HB + 1):
        along_lon = along_lon + filter_taps[:, tap_number, None, None] * jnp.roll(source, HB - tap_number, axis=2)
    padded = jnp.pad(along_lon, ((0, 0), (HB, HB), (0, 0)))
    result = jnp.zeros_like(source)
    for tap_number in range(2 * HB + 1):
        result = result + filter_taps[:, tap_number, None, None] * padded[:, tap_number:tap_number + NCLAT, :]
    return result

def reference(alpha_fields, member_perts, band_widths, lat_index, lat_weight, lon_index, lon_weight, innovation, obs_weight):
    filter_taps = tap_table(band_widths)

    def accumulate(running, member_pair):
        localized = localize(member_pair[0].astype(jnp.float32), filter_taps)
        return (running + member_pair[1].astype(jnp.float32) * localized, None)
    coarse_increment, unused = lax.scan(accumulate, jnp.zeros((LEV, NCLAT, NCLON), jnp.float32), (alpha_fields, member_perts))
    lat_next = (lat_index + 1).astype(jnp.int32)
    lon_next = jnp.remainder(lon_index + 1, NCLON).astype(jnp.int32)
    north_weight = lat_weight[None, :, None]
    east_weight = lon_weight[None, None, :]
    by_lat = (1.0 - north_weight) * coarse_increment[:, lat_index, :] + north_weight * coarse_increment[:, lat_next, :]
    increment = (1.0 - east_weight) * by_lat[:, :, lon_index] + east_weight * by_lat[:, :, lon_next]
    misfit = obs_weight * (increment - innovation)
    spread_lon = jnp.zeros((LEV, NFLAT, NCLON), jnp.float32)
    spread_lon = spread_lon.at[:, :, lon_index].add((1.0 - east_weight) * misfit)
    spread_lon = spread_lon.at[:, :, lon_next].add(east_weight * misfit)
    coarse_residual = jnp.zeros((LEV, NCLAT, NCLON), jnp.float32)
    coarse_residual = coarse_residual.at[:, lat_index, :].add((1.0 - north_weight) * spread_lon)
    coarse_residual = coarse_residual.at[:, lat_next, :].add(north_weight * spread_lon)

    def member_gradient(member_pair):
        product = member_pair[1].astype(jnp.float32) * coarse_residual
        return member_pair[0].astype(jnp.float32) + localize(product, filter_taps)
    gradient = lax.map(member_gradient, (alpha_fields, member_perts))
    return (increment, gradient)
```

```python
import functools

import jax
import jax.numpy as jnp
from jax import lax
from jax.experimental import pallas as pl
from jax.experimental.pallas import tpu as pltpu
from jax.sharding import PartitionSpec as P

HB = 8
GROUP = 16
MEMBERS = 8
LANES = 128
HIGHEST = lax.Precision.HIGHEST
F32 = jnp.float32
BF16 = jnp.bfloat16


def rounded(size, step):
    return -(-size // step) * step


def iota(shape, axis):
    return lax.broadcasted_iota(jnp.int32, shape, axis)


def split(value):
    high = value.astype(BF16)
    return high, (value - high.astype(F32)).astype(BF16)


def dot(left, right, precision=None):
    return lax.dot_general(
        left, right, (((1,), (0,)), ((), ())), precision=precision, preferred_element_type=F32
    )


def row_of(index, height):
    above = index - height - HB
    return jnp.where(index < height, index, jnp.where(index < height + HB, above, index - HB))


def packed_column(lane, level, width):
    west = (lane < LANES // 2) if level == 0 else (lane >= LANES // 2)
    cell = lane % HB
    return jnp.where(west, cell - HB, width + cell)


def packed_member(lane):
    return (lane % (LANES // 2)) // HB


def taps(offset, spread):
    lane = iota((8, LANES), 1)
    distance = (lane - HB).astype(F32)
    scale = jnp.full((8, LANES), 1.0, F32) * (0.5 / (spread * spread))
    shape = jnp.where(lane <= 2 * HB, jnp.exp(-(distance * distance) * scale), 0.0)
    norm = lax.rsqrt(jnp.sum(shape * shape, axis=1, keepdims=True))[:1, :1]
    far = offset.astype(F32)
    value = jnp.exp(-(far * far) * scale[:1, :1]) * norm
    return jnp.where(jnp.abs(offset) <= HB, value, 0.0)


def pack_kernel(perts_ref, halo_ref, east_ref, west_ref):
    rows = east_ref.shape[1]
    width = perts_ref.shape[2]
    lane = iota((rows, LANES), 1)
    east = jnp.zeros((rows, LANES), F32)
    west = jnp.zeros((rows, LANES), F32)
    for k in range(GROUP):
        t, level = k // 2, k % 2
        own = perts_ref[k]
        halo = halo_ref[k]
        last = jnp.concatenate([own[:, width - LANES :], halo[:, width - LANES :]], 0).astype(F32)
        first = jnp.concatenate([own[:, :LANES], halo[:, :LANES]], 0).astype(F32)
        slot = level * (LANES // 2) + t * HB
        other = (1 - level) * (LANES // 2) + t * HB
        last = pltpu.roll(last, (slot + HB) % LANES, 1)
        first = first if other == 0 else pltpu.roll(first, other, 1)
        east = jnp.where(lane // HB == slot // HB, last, east)
        west = jnp.where(lane // HB == other // HB, first, west)
    east_ref[0] = east.astype(BF16)
    west_ref[0] = west.astype(BF16)


def local_kernel(
    width_ref, alpha_ref, perts_ref, sum_ref, rows_ref, cols_ref, lon_ref, lat_ref, stack_ref
):
    height, width = alpha_ref.shape[1], alpha_ref.shape[2]
    ext = height + 2 * HB

    @pl.when(pl.program_id(0) == 0)
    def _():
        sum_ref[...] = jnp.zeros_like(sum_ref)
        for level in range(2):
            spread = width_ref[level].astype(F32)
            source = iota((width, width), 0)
            high, low = split(taps(source - iota((width, width), 1), spread))
            source = iota((width, LANES), 0)
            lane = iota((width, LANES), 1)
            edge = taps(source - packed_column(lane, level, width), spread)
            for t in range(MEMBERS):
                part_high, part_low = split(jnp.where(packed_member(lane) == t, edge, 0.0))
                lon_ref[level, t, :width, :width] = high
                lon_ref[level, t, width:, :width] = low
                lon_ref[level, t, :width, width:] = part_high
                lon_ref[level, t, width:, width:] = part_low
            target = row_of(iota((ext, height), 0), height)
            high, low = split(taps(target - iota((ext, height), 1), spread))
            lat_ref[level, :, :height] = high
            lat_ref[level, :, height : 2 * height] = low
            lat_ref[level, :, 2 * height :] = high

    for level in range(2):
        packed = jnp.zeros((height, LANES), F32)
        for t in range(MEMBERS):
            field = alpha_ref[2 * t + level]
            both = dot(jnp.concatenate([field, field], 1), lon_ref[level, t])
            high, low = split(both[:, :width])
            stack_ref[:height, t * width : (t + 1) * width] = high
            stack_ref[height : 2 * height, t * width : (t + 1) * width] = high
            stack_ref[2 * height :, t * width : (t + 1) * width] = low
            packed = packed + both[:, width:]
        high, low = split(packed)
        stack_ref[:height, MEMBERS * width :] = high
        stack_ref[height : 2 * height, MEMBERS * width :] = high
        stack_ref[2 * height :, MEMBERS * width :] = low
        total = sum_ref[level]
        for pair in range(MEMBERS // 2):
            base = 2 * pair * width
            wide = dot(lat_ref[level], stack_ref[:, base : base + 2 * width])
            for side in range(2):
                k = 2 * (2 * pair + side) + level
                field = wide[:, side * width : (side + 1) * width]
                total = total + perts_ref[k].astype(F32) * field[:height]
                rows_ref[k] = field[height:]
        sum_ref[level] = total
        cols_ref[0, level] = dot(lat_ref[level], stack_ref[:, MEMBERS * width :])


def frame_kernel(sum_ref, rows_ref, cols_ref, halo_ref, west_ref, east_ref, out_ref):
    height, width = sum_ref.shape[1], sum_ref.shape[2]
    ext = height + 2 * HB
    groups = west_ref.shape[0]
    lane = iota((ext, LANES), 1)
    out = out_ref.shape[2]
    for level in range(2):
        edge = jnp.zeros((2 * HB, width), F32)
        packed = jnp.zeros((ext, LANES), F32)
        for group in range(groups):
            for t in range(MEMBERS):
                k = group * GROUP + 2 * t + level
                edge = edge + halo_ref[k].astype(F32) * rows_ref[k]
            west = west_ref[group].astype(F32)
            east = east_ref[group].astype(F32)
            half = lane < LANES // 2
            cell = jnp.where(half, west, east) if level == 0 else jnp.where(half, east, west)
            packed = packed + cell * cols_ref[group, level]
        own = jnp.concatenate([edge[:HB], sum_ref[level], edge[HB:]], 0)
        packed = jnp.concatenate(
            [packed[height : height + HB], packed[:height], packed[height + HB :]], 0
        )
        place = (iota((width, out), 0) + HB == iota((width, out), 1)).astype(F32)
        column = packed_column(iota((LANES, out), 0), level, width)
        gather = (column + HB == iota((LANES, out), 1)).astype(F32)
        out_ref[level] = dot(own, place, HIGHEST) + dot(packed, gather, HIGHEST)


def fine_kernel(
    margin,
    coarse_ref,
    target_ref,
    weight_ref,
    lat_col_ref,
    lat_row_ref,
    lon_col_ref,
    lon_row_ref,
    inc_ref,
    own_ref,
    edge_ref,
):
    height, width = own_ref.shape[1] - 2 * HB, own_ref.shape[2]
    ext = height + 2 * HB
    fine_rows, fine_cols = target_ref.shape[1], target_ref.shape[2]
    coarse_rows, coarse_cols = coarse_ref.shape[1], coarse_ref.shape[2]
    tall = lat_row_ref.shape[1]
    skirt = 2 * margin - 2

    def interpolate(cell, index, weight):
        near = jnp.where(cell == index, 1.0 - weight, 0.0)
        return near + jnp.where(cell == index + 1, weight, 0.0)

    lat_index = lat_col_ref[:, 0:1].astype(jnp.int32)
    lat_map = interpolate(iota((fine_rows, coarse_rows), 1), lat_index, lat_col_ref[:, 1:2])
    lon_index = lon_row_ref[0:1, :].astype(jnp.int32)
    lon_map = interpolate(iota((coarse_cols, fine_cols), 0), lon_index, lon_row_ref[1:2, :])
    row = row_of(iota((ext, tall), 0), height) + margin
    lat_index = lat_row_ref[0:1, :].astype(jnp.int32)
    lat_back = interpolate(row, lat_index, lat_row_ref[1:2, :])
    back_index = lon_col_ref[:, 0:1].astype(jnp.int32)
    back_weight = lon_col_ref[:, 1:2]
    own_back = interpolate(iota((fine_cols, width), 1) + margin, back_index, back_weight)
    for level in range(2):
        by_lat = dot(lat_map, coarse_ref[level], HIGHEST)
        increment = dot(by_lat, lon_map, HIGHEST)
        rows, cols = inc_ref.shape[1], inc_ref.shape[2]
        inc_ref[level] = increment[skirt : skirt + rows, skirt : skirt + cols]
        misfit = weight_ref[level] * (increment - target_ref[level])
        column = packed_column(iota((fine_cols, LANES), 1), level, width) + margin
        edge_back = interpolate(column, back_index, back_weight)
        lon_back = dot(misfit, jnp.concatenate([own_back, edge_back], 1), HIGHEST)
        if tall > fine_rows:
            blank = jnp.zeros((tall - fine_rows, width + LANES), F32)
            lon_back = jnp.concatenate([lon_back, blank], 0)
        residual = dot(lat_back, lon_back, HIGHEST)
        own_ref[level] = residual[:, :width]
        edge_ref[level] = residual[:, width:]


def gradient_kernel(
    width_ref, alpha_ref, perts_ref, halo_ref, west_ref, east_ref, own_ref, edge_ref, out_ref,
    lon_ref, lat_ref, stack_ref,
):
    height, width = alpha_ref.shape[1], alpha_ref.shape[2]
    ext = height + 2 * HB

    @pl.when(pl.program_id(0) == 0)
    def _():
        for level in range(2):
            spread = width_ref[level].astype(F32)
            source = iota((width, width), 0)
            high, low = split(taps(source - iota((width, width), 1), spread))
            lane = iota((LANES, width), 0)
            edge = taps(packed_column(lane, level, width) - iota((LANES, width), 1), spread)
            for t in range(MEMBERS):
                part_high, part_low = split(jnp.where(packed_member(lane) == t, edge, 0.0))
                lon_ref[level, t, :width, :width] = high
                lon_ref[level, t, :width, width:] = low
                lon_ref[level, t, width:, :width] = part_high
                lon_ref[level, t, width:, width:] = part_low
            source = row_of(iota((height, ext), 1), height)
            high, low = split(taps(source - iota((height, ext), 0), spread))
            lat_ref[level, :, :ext] = high
            lat_ref[level, :, ext : 2 * ext] = low
            lat_ref[level, :, 2 * ext :] = high

    half = iota((ext, LANES), 1) < LANES // 2
    west = west_ref[0].astype(F32)
    east = east_ref[0].astype(F32)

    def stack(value, start, size):
        high, low = split(value)
        stack_ref[:ext, start : start + size] = high
        stack_ref[ext : 2 * ext, start : start + size] = high
        stack_ref[2 * ext :, start : start + size] = low

    for level in range(2):
        cell = jnp.where(half, west, east) if level == 0 else jnp.where(half, east, west)
        stack(cell * edge_ref[level], MEMBERS * width, LANES)
        for t in range(MEMBERS):
            k = 2 * t + level
            field = jnp.concatenate([perts_ref[k], halo_ref[k]], 0).astype(F32)
            stack(field * own_ref[level], t * width, width)
        edge_high, edge_low = split(dot(lat_ref[level], stack_ref[:, MEMBERS * width :]))
        for pair in range(MEMBERS // 2):
            base = 2 * pair * width
            wide = dot(lat_ref[level], stack_ref[:, base : base + 2 * width])
            for side in range(2):
                t = 2 * pair + side
                k = 2 * t + level
                high, low = split(wide[:, side * width : (side + 1) * width])
                main = dot(jnp.concatenate([high, edge_high], 1), lon_ref[level, t])
                rest = dot(jnp.concatenate([low, edge_low], 1), lon_ref[level, t, :, :width])
                total = main[:, :width] + main[:, width:] + rest
                out_ref[k] = alpha_ref[k].astype(F32) + total


def ring(axis, periodic):
    count = lax.axis_size(axis)
    forward = [(i, i + 1) for i in range(count - 1)]
    if periodic:
        forward.append((count - 1, 0))
    return forward, [(target, source) for source, target in forward]


def exchange(to_next, to_previous, axis, periodic):
    forward, backward = ring(axis, periodic)
    return lax.ppermute(to_next, axis, forward), lax.ppermute(to_previous, axis, backward)


def vmem(*shape):
    return pl.BlockSpec(shape, lambda s: (0,) * len(shape))


def grouped(*shape):
    return pl.BlockSpec(shape, lambda s: (s,) + (0,) * (len(shape) - 1))


def params(*semantics):
    return pltpu.CompilerParams(dimension_semantics=semantics, vmem_limit_bytes=60 * 1024 * 1024)


def body(
    alpha_fields,
    member_perts,
    band_widths,
    lat_index,
    lat_weight,
    lon_index,
    lon_weight,
    innovation,
    obs_weight,
):
    members, levels, height, width = alpha_fields.shape
    fields = members * levels
    groups = fields // GROUP
    ext = height + 2 * HB
    margin = HB + 2
    skirt = 2 * margin - 2
    strip = margin + HB
    fine_h, fine_w = innovation.shape[1], innovation.shape[2]
    alpha = alpha_fields.reshape(fields, height, width)
    perts = member_perts.reshape(fields, height, width)
    smem = pl.BlockSpec(memory_space=pltpu.SMEM)

    above, below = exchange(perts[:, height - HB :], perts[:, :HB], "gy", False)
    halo = jnp.concatenate([above, below], axis=1)
    east_send, west_send = pl.pallas_call(
        pack_kernel,
        grid=(groups,),
        in_specs=[grouped(GROUP, height, width), grouped(GROUP, 2 * HB, width)],
        out_specs=[grouped(1, ext, LANES)] * 2,
        out_shape=[jax.ShapeDtypeStruct((groups, ext, LANES), BF16)] * 2,
        compiler_params=params("arbitrary"),
        name="pack",
    )(perts, halo)
    west, east = exchange(east_send, west_send, "gx", True)

    lane = jnp.arange(fine_w)[None, :]
    table = jnp.where(
        lane == 0,
        lat_index.astype(F32)[:, None],
        jnp.where(lane == 1, lat_weight[:, None], 0.0),
    )[None]

    def rows_of(cut):
        return jnp.concatenate([innovation[:, cut], obs_weight[:, cut], table[:, cut]], 0)

    top, bottom = exchange(
        rows_of(slice(fine_h - skirt, None)), rows_of(slice(0, skirt)), "gy", False
    )
    target = jnp.concatenate([top[:2], innovation, bottom[:2]], 1)
    weight = jnp.concatenate([top[2:4], obs_weight, bottom[2:4]], 1)
    lat_table = jnp.concatenate([top[4, :, :2], table[0, :, :2], bottom[4, :, :2]], 0)
    tall = fine_h + 2 * skirt
    row = jnp.arange(tall)[:, None]

    def cols_of(cut):
        lon = jnp.where(
            row == 0, lon_index.astype(F32)[None, cut], jnp.where(row == 1, lon_weight[None, cut], 0.0)
        )[None]
        return jnp.concatenate([target[:, :, cut], weight[:, :, cut], lon], 0)

    left, right = exchange(
        cols_of(slice(fine_w - skirt, None)), cols_of(slice(0, skirt)), "gx", True
    )
    pad_rows = rounded(tall, 8) - tall
    pad_cols = rounded(fine_w + 2 * skirt, LANES) - fine_w - 2 * skirt
    pads = ((0, 0), (0, pad_rows), (0, pad_cols))
    target = jnp.pad(jnp.concatenate([left[:2], target, right[:2]], 2), pads)
    weight = jnp.pad(jnp.concatenate([left[2:4], weight, right[2:4]], 2), pads)
    lon_table = jnp.concatenate(
        [left[4, :2], jnp.stack([lon_index.astype(F32), lon_weight]), right[4, :2]], 1
    )
    lat_start = lax.axis_index("gy") * height
    lon_start = lax.axis_index("gx") * width
    lon_total = width * lax.axis_size("gx")
    lat_rel = lat_table[:, 0] - (lat_start - margin).astype(F32)
    lon_rel = jnp.remainder(
        lon_table[0].astype(jnp.int32) - lon_start + margin, lon_total
    ).astype(F32)

    def padded(index, values, size):
        short = size - index.shape[0]
        index = jnp.pad(index, (0, short), constant_values=-9.0)
        return jnp.stack([index, jnp.pad(values, (0, short))])

    lat_col = padded(lat_rel, lat_table[:, 1], tall + pad_rows).T
    lat_row = padded(lat_rel, lat_table[:, 1], rounded(tall, LANES))
    lon_row = padded(lon_rel, lon_table[1], fine_w + 2 * skirt + pad_cols)
    lon_col = lon_row.T

    partial, edge_rows, edge_cols = pl.pallas_call(
        local_kernel,
        grid=(groups,),
        in_specs=[smem, grouped(GROUP, height, width), grouped(GROUP, height, width)],
        out_specs=[
            vmem(2, height, width),
            grouped(GROUP, 2 * HB, width),
            grouped(1, 2, ext, LANES),
        ],
        out_shape=[
            jax.ShapeDtypeStruct((2, height, width), F32),
            jax.ShapeDtypeStruct((fields, 2 * HB, width), F32),
            jax.ShapeDtypeStruct((groups, 2, ext, LANES), F32),
        ],
        scratch_shapes=[
            pltpu.VMEM((2, MEMBERS, 2 * width, width + LANES), BF16),
            pltpu.VMEM((2, ext, 3 * height), BF16),
            pltpu.VMEM((3 * height, MEMBERS * width + LANES), BF16),
        ],
        compiler_params=params("arbitrary"),
        name="local",
        cost_estimate=pl.CostEstimate(flops=10**10, bytes_accessed=10**7, transcendentals=0),
    )(band_widths, alpha, perts)

    framed = pl.pallas_call(
        frame_kernel,
        out_shape=jax.ShapeDtypeStruct((2, ext, width + 2 * HB), F32),
        compiler_params=params(),
        name="frame",
    )(partial, edge_rows, edge_cols, halo, west, east)
    count = lax.axis_size("ma")
    swap = [(i, (i + 1) % count) for i in range(count)]
    framed = framed + lax.ppermute(framed, "ma", swap)
    above, below = exchange(framed[:, ext - strip :], framed[:, :strip], "gy", False)
    gap = ext + 4 - strip
    framed = (
        jnp.pad(framed, ((0, 0), (2, 2), (0, 0)))
        + jnp.pad(above, ((0, 0), (0, gap), (0, 0)))
        + jnp.pad(below, ((0, 0), (gap, 0), (0, 0)))
    )
    wide = framed.shape[2]
    before, after = exchange(framed[:, :, wide - strip :], framed[:, :, :strip], "gx", True)
    rows = rounded(ext + 4, LANES)
    cols = rounded(wide + 4, LANES)
    gap = wide + 4 - strip

    def place(value, start):
        return jnp.pad(
            value,
            ((0, 0), (0, rows - value.shape[1]), (start, cols - start - value.shape[2])),
        )

    coarse = place(framed, 2) + place(before, 0) + place(after, gap)
    increment, own, edge = pl.pallas_call(
        functools.partial(fine_kernel, margin),
        out_shape=[
            jax.ShapeDtypeStruct((2, fine_h, fine_w), F32),
            jax.ShapeDtypeStruct((2, ext, width), F32),
            jax.ShapeDtypeStruct((2, ext, LANES), F32),
        ],
        compiler_params=params(),
        name="fine",
    )(coarse, target, weight, lat_col, lat_row, lon_col, lon_row)

    gradient = pl.pallas_call(
        gradient_kernel,
        grid=(groups,),
        in_specs=[
            smem,
            grouped(GROUP, height, width),
            grouped(GROUP, height, width),
            grouped(GROUP, 2 * HB, width),
            grouped(1, ext, LANES),
            grouped(1, ext, LANES),
            vmem(2, ext, width),
            vmem(2, ext, LANES),
        ],
        out_specs=grouped(GROUP, height, width),
        out_shape=jax.ShapeDtypeStruct((fields, height, width), F32),
        scratch_shapes=[
            pltpu.VMEM((2, MEMBERS, width + LANES, 2 * width), BF16),
            pltpu.VMEM((2, height, 3 * ext), BF16),
            pltpu.VMEM((3 * ext, MEMBERS * width + LANES), BF16),
        ],
        compiler_params=params("arbitrary"),
        name="gradient",
    )(band_widths, alpha, perts, halo, west, east, own, edge)
    return increment, gradient.reshape(alpha_fields.shape)


def solution(mesh):
    placed = (
        P("ma", None, "gy", "gx"),
        P("ma", None, "gy", "gx"),
        P(),
        P("gy"),
        P("gy"),
        P("gx"),
        P("gx"),
        P(None, "gy", "gx"),
        P(None, "gy", "gx"),
    )
    return jax.shard_map(
        body,
        mesh=mesh,
        in_specs=placed,
        out_specs=(P(None, "gy", "gx"), P("ma", None, "gy", "gx")),
        check_vma=False,
    )
```

```python
import functools

import jax
import jax.numpy as jnp
from jax import lax
from jax.experimental import pallas as pl
from jax.experimental.pallas import tpu as pltpu
from jax.sharding import PartitionSpec as P

HB = 8
GROUP = 16
MEMBERS = 8
SKIRT = 24
STRIP = 24
NOWHERE = -9999
LANES = 128
F32 = jnp.float32
BF16 = jnp.bfloat16


def rounded(size, step):
    return -(-size // step) * step


def iota(shape, axis):
    return lax.broadcasted_iota(jnp.int32, shape, axis)


def split(value):
    high = value.astype(BF16)
    return high, (value - high.astype(F32)).astype(BF16)


def dot(left, right, dims=(1, 0)):
    return lax.dot_general(
        left, right, (((dims[0],), (dims[1],)), ((), ())), preferred_element_type=F32
    )


def dot3(left, right, dims=(1, 0)):
    left_high, left_low = split(left)
    right_high, right_low = split(right)
    total = dot(left_high, right_low, dims) + dot(left_low, right_high, dims)
    return total + dot(left_high, right_high, dims)


def row_of(index, height):
    above = index - height - HB
    return jnp.where(index < height, index, jnp.where(index < height + HB, above, index - HB))


def packed_column(lane, level, width):
    west = (lane < LANES // 2) if level == 0 else (lane >= LANES // 2)
    cell = lane & (HB - 1)
    return jnp.where(west, cell - HB, width + cell)


def packed_member(lane):
    return (lane & (LANES // 2 - 1)) >> 3


def taps(offset, spread):
    lane = iota((8, LANES), 1)
    distance = (lane - HB).astype(F32)
    scale = jnp.full((8, LANES), 1.0, F32) * (0.5 / (spread * spread))
    shape = jnp.where(lane <= 2 * HB, jnp.exp(-(distance * distance) * scale), 0.0)
    norm = lax.rsqrt(jnp.sum(shape * shape, axis=1, keepdims=True))[:1, :1]
    far = offset.astype(F32)
    value = jnp.exp(-(far * far) * scale[:1, :1]) * norm
    return jnp.where(jnp.abs(offset) <= HB, value, 0.0)


def pack_kernel(perts_ref, above_ref, below_ref, east_ref, west_ref):
    rows = east_ref.shape[1]
    width = perts_ref.shape[2]
    lane = iota((rows, LANES), 1)
    east = jnp.zeros((rows, LANES), F32)
    west = jnp.zeros((rows, LANES), F32)
    for k in range(GROUP):
        t, level = k // 2, k % 2
        own = perts_ref[k]
        whole = jnp.concatenate(
            [own.astype(F32), above_ref[k].astype(F32), below_ref[k].astype(F32)], 0
        )
        last = whole[:, width - LANES :]
        first = whole[:, :LANES]
        slot = level * (LANES // 2) + t * HB
        other = (1 - level) * (LANES // 2) + t * HB
        last = pltpu.roll(last, (slot + HB) % LANES, 1)
        first = first if other == 0 else pltpu.roll(first, other, 1)
        east = jnp.where(lane >> 3 == slot // HB, last, east)
        west = jnp.where(lane >> 3 == other // HB, first, west)
    east_ref[0] = east.astype(BF16)
    west_ref[0] = west.astype(BF16)


def local_kernel(
    width_ref, alpha_ref, perts_ref, token_ref, sum_ref, rows_ref, cols_ref, lon_ref, lat_ref, stack_ref
):
    height, width = alpha_ref.shape[1], alpha_ref.shape[2]
    ext = height + 2 * HB

    @pl.when(pl.program_id(0) == 0)
    def _():
        sum_ref[...] = jnp.zeros_like(sum_ref)
        for level in range(2):
            spread = width_ref[level].astype(F32)
            source = iota((width, width), 0)
            high, low = split(taps(source - iota((width, width), 1), spread))
            source = iota((width, LANES), 0)
            lane = iota((width, LANES), 1)
            edge = taps(source - packed_column(lane, level, width), spread)
            for t in range(MEMBERS):
                part_high, part_low = split(jnp.where(packed_member(lane) == t, edge, 0.0))
                lon_ref[level, t, :width, :width] = high
                lon_ref[level, t, width:, :width] = low
                lon_ref[level, t, :width, width:] = part_high
                lon_ref[level, t, width:, width:] = part_low
            target = row_of(iota((ext, height), 0), height)
            high, low = split(taps(target - iota((ext, height), 1), spread))
            lat_ref[level, :, :height] = high
            lat_ref[level, :, height : 2 * height] = low
            lat_ref[level, :, 2 * height :] = high

    for level in range(2):
        packed = jnp.zeros((height, LANES), F32)
        for t in range(MEMBERS):
            field = alpha_ref[2 * t + level]
            both = dot(jnp.concatenate([field, field], 1), lon_ref[level, t])
            high, low = split(both[:, :width])
            stack_ref[:height, t * width : (t + 1) * width] = high
            stack_ref[height : 2 * height, t * width : (t + 1) * width] = high
            stack_ref[2 * height :, t * width : (t + 1) * width] = low
            packed = packed + both[:, width:]
        high, low = split(packed)
        stack_ref[:height, MEMBERS * width :] = high
        stack_ref[height : 2 * height, MEMBERS * width :] = high
        stack_ref[2 * height :, MEMBERS * width :] = low
        total = sum_ref[level]
        for pair in range(MEMBERS // 2):
            base = 2 * pair * width
            wide = dot(lat_ref[level], stack_ref[:, base : base + 2 * width])
            for side in range(2):
                k = 2 * (2 * pair + side) + level
                field = wide[:, side * width : (side + 1) * width]
                total = total + perts_ref[k].astype(F32) * field[:height]
                rows_ref[k] = field[height:]
        sum_ref[level] = total
        cols_ref[0, level] = dot(lat_ref[level], stack_ref[:, MEMBERS * width :])


def stacked_cell(index, size, base):
    cell = row_of(index, size)
    low = index - base
    cell = jnp.where(index < size + 2 * HB, cell, NOWHERE)
    cell = jnp.where((low >= 0) & (low < STRIP), low - 2 * HB, cell)
    return jnp.where((low >= STRIP) & (low < 2 * STRIP), low - STRIP + size - HB, cell)


def interpolate(cell, index, weight):
    near = jnp.where(cell == index, 1.0 - weight, 0.0)
    return near + jnp.where(cell == index + 1, weight, 0.0)


def rows_kernel(last_ref, first_ref, next_ref, previous_ref):
    next_ref[...] = last_ref[...]
    previous_ref[...] = first_ref[...]


def table(index, weight):
    size = index.shape[-1]
    row = iota((8, size), 0)
    return jnp.where(
        row == 0, index.astype(F32).reshape(1, size), jnp.where(row == 1, weight.reshape(1, size), 0.0)
    )


def fine_cols_kernel(target_ref, weight_ref, index_ref, share_ref, east_ref, west_ref):
    cols = target_ref.shape[2]
    for a, ref in enumerate((target_ref, weight_ref)):
        for level in range(2):
            start = (2 * a + level) * SKIRT
            east_ref[start : start + SKIRT] = ref[level, :, cols - LANES :].T[LANES - SKIRT :]
            west_ref[start : start + SKIRT] = ref[level, :, :LANES].T[:SKIRT]
    lon = table(index_ref[...], share_ref[...])
    east_ref[4 * SKIRT :, :LANES] = lon[:, cols - LANES :]
    west_ref[4 * SKIRT :, :LANES] = lon[:, :LANES]


def fine_rows_kernel(
    target_ref, weight_ref, index_ref, share_ref, west_ref, east_ref, next_ref, previous_ref, token_ref
):
    rows = target_ref.shape[1]
    for a, ref in enumerate((target_ref, weight_ref)):
        for level in range(2):
            start = (2 * a + level) * SKIRT
            next_ref[start : start + SKIRT] = ref[level, rows - SKIRT :]
            previous_ref[start : start + SKIRT] = ref[level, :SKIRT]
    lat = table(index_ref[...], share_ref[...])
    for side, ref in enumerate((west_ref, east_ref)):
        lanes = slice(side * LANES, (side + 1) * LANES)
        next_ref[4 * SKIRT : 8 * SKIRT, lanes] = ref[: 4 * SKIRT, rows - LANES :]
        previous_ref[4 * SKIRT : 8 * SKIRT, lanes] = ref[: 4 * SKIRT, :LANES]
    next_ref[8 * SKIRT :, :LANES] = lat[:, rows - LANES :]
    previous_ref[8 * SKIRT :, :LANES] = lat[:, :LANES]
    token_ref[...] = lat[:, :LANES]


def frame_kernel(sum_ref, rows_ref, cols_ref, above_ref, below_ref, west_ref, east_ref, out_ref):
    height, width = sum_ref.shape[1], sum_ref.shape[2]
    ext = height + 2 * HB
    groups = west_ref.shape[0]
    half = iota((ext, LANES), 1) < LANES // 2
    for level in range(2):
        edge = jnp.zeros((2 * HB, width), F32)
        packed = jnp.zeros((ext, LANES), F32)
        for group in range(groups):
            for t in range(MEMBERS):
                k = group * GROUP + 2 * t + level
                halo = jnp.concatenate([above_ref[k].astype(F32), below_ref[k].astype(F32)], 0)
                edge = edge + halo * rows_ref[k]
            west = west_ref[group].astype(F32)
            east = east_ref[group].astype(F32)
            cell = jnp.where(half, west, east) if level == 0 else jnp.where(half, east, west)
            packed = packed + cell * cols_ref[group, level]
        column = packed_column(iota((LANES, LANES), 0), level, width)
        slot = iota((LANES, LANES), 1)
        target = jnp.where(slot < HB, slot - HB, jnp.where(slot < 2 * HB, slot - HB + width, NOWHERE))
        gather = (column == target).astype(BF16)
        high, low = split(packed)
        out_ref[level, :height, :width] = sum_ref[level]
        out_ref[level, height:, :width] = edge
        out_ref[level, :, width:] = dot(high, gather) + dot(low, gather)


def total_kernel(mine_ref, other_ref, total_ref, next_ref, previous_ref):
    total = mine_ref[...] + other_ref[...]
    height = total.shape[1] - 2 * HB
    total_ref[...] = total
    next_ref[:, : 2 * HB] = total[:, height - 2 * HB : height]
    next_ref[:, 2 * HB :] = total[:, height + HB :]
    previous_ref[:, :HB] = total[:, height : height + HB]
    previous_ref[:, HB:] = total[:, : 2 * HB]


def strips_kernel(width, total_ref, above_ref, below_ref, stack_ref, east_ref, west_ref):
    ext, lanes = total_ref.shape[1], total_ref.shape[2]
    rows = stack_ref.shape[1]
    column = stacked_cell(iota((STRIP, lanes), 1), width, lanes)
    number = iota((STRIP, lanes), 0)
    pick_east = (column == number + width - 2 * HB).astype(BF16)
    pick_west = (column == number - HB).astype(BF16)
    for level in range(2):
        stack_ref[level, :ext] = total_ref[level]
        stack_ref[level, ext : ext + STRIP] = above_ref[level]
        stack_ref[level, ext + STRIP : ext + 2 * STRIP] = below_ref[level]
        stack_ref[level, ext + 2 * STRIP :] = jnp.zeros((rows - ext - 2 * STRIP, lanes), F32)
        high, low = split(stack_ref[level])
        part = slice(level * STRIP, (level + 1) * STRIP)
        east_ref[part] = dot(pick_east, high, (1, 1)) + dot(pick_east, low, (1, 1))
        west_ref[part] = dot(pick_west, high, (1, 1)) + dot(pick_west, low, (1, 1))


def fine_kernel(
    lon_total,
    start_ref,
    stack_ref,
    strip_west_ref,
    strip_east_ref,
    target_ref,
    weight_ref,
    lat_index_ref,
    lat_share_ref,
    lon_index_ref,
    lon_share_ref,
    west_ref,
    east_ref,
    above_ref,
    below_ref,
    inc_ref,
    own_ref,
    edge_ref,
    wide_ref,
    miss_ref,
):
    ext, width = own_ref.shape[1], own_ref.shape[2]
    height = ext - 2 * HB
    rows, cols = target_ref.shape[1], target_ref.shape[2]
    lanes = stack_ref.shape[2]
    span = rows + LANES
    lane = iota((8, LANES), 1)
    first = iota((8, LANES), 0) == 0

    def side(low, high):
        low = pltpu.roll(low, SKIRT, 1)
        high = pltpu.roll(high, SKIRT, 1)
        blank = jnp.where(first, 1.0e6, 0.0)
        return jnp.where(lane < SKIRT, low, jnp.where(lane < 2 * SKIRT, high, blank))

    def corner(low, high):
        spot = iota(low.shape, 1)
        low = pltpu.roll(low, SKIRT, 1)
        high = pltpu.roll(high, SKIRT, 1)
        return jnp.where(spot < SKIRT, low, jnp.where(spot < 2 * SKIRT, high, 0.0))

    lat_side = side(above_ref[8 * SKIRT :, :LANES], below_ref[8 * SKIRT :, :LANES])
    lat = jnp.concatenate([table(lat_index_ref[...], lat_share_ref[...]), lat_side], 1)
    lon_side = side(west_ref[4 * SKIRT :, :LANES], east_ref[4 * SKIRT :, :LANES])
    lon = jnp.concatenate([table(lon_index_ref[...], lon_share_ref[...]), lon_side], 1)
    lat_cell = lat[0:1].astype(jnp.int32) - start_ref[0]
    lat_share = lat[1:2]
    lon_cell = lon[0:1].astype(jnp.int32) - start_ref[1]
    lon_cell = jnp.where(lon_cell < -(lon_total // 2), lon_cell + lon_total, lon_cell)
    wrap = (lon_cell >= lon_total // 2) & (lon_cell < lon_total)
    lon_cell = jnp.where(wrap, lon_cell - lon_total, lon_cell)
    lon_share = lon[1:2]
    upright = jnp.concatenate([lat_cell.astype(F32), lat_share, jnp.zeros((6, span), F32)], 0).T
    lat_cell_up, lat_share_up = upright[:, 0:1].astype(jnp.int32), upright[:, 1:2]
    upright = jnp.concatenate(
        [lon_cell.astype(F32), lon_share, jnp.zeros((6, cols + LANES), F32)], 0
    ).T
    lon_cell_up, lon_share_up = upright[:, 0:1].astype(jnp.int32), upright[:, 1:2]
    beside = slice(cols, cols + 2 * SKIRT)

    tall = stack_ref.shape[1]
    lat_map = interpolate(
        stacked_cell(iota((span, tall), 1), height, ext), lat_cell_up, lat_share_up
    )
    broad = lanes + LANES
    lon_map = interpolate(
        stacked_cell(iota((broad, cols), 0), width, lanes), lon_cell[:, :cols], lon_share[:, :cols]
    )
    side_map = interpolate(
        stacked_cell(iota((2 * SKIRT, broad), 1), width, lanes),
        lon_cell_up[beside],
        lon_share_up[beside],
    )
    lat_back = interpolate(row_of(iota((ext, span), 0), height), lat_cell, lat_share)
    lat_high, lat_low = split(lat_map)
    wide_ref[:, lanes:] = jnp.zeros((span, LANES), F32)
    miss_ref[rows + 2 * SKIRT :] = jnp.zeros((span - rows - 2 * SKIRT, cols), F32)

    for level in range(2):
        wide_ref[:, :lanes] = dot3(lat_map, stack_ref[level])
        part = slice(level * STRIP, (level + 1) * STRIP)
        strips = jnp.concatenate([strip_west_ref[part], strip_east_ref[part]], 0)
        wide_ref[:, lanes : lanes + 2 * STRIP] = dot3(lat_map, strips, (1, 1))
        increment = dot3(wide_ref[...], lon_map)
        inc_ref[level] = increment[:rows]
        miss_ref[:rows] = weight_ref[level] * (increment[:rows] - target_ref[level])
        target_rows = slice(level * SKIRT, (level + 1) * SKIRT)
        weight_rows = slice((2 + level) * SKIRT, (3 + level) * SKIRT)
        for number, ref in enumerate((above_ref, below_ref)):
            start = rows + number * SKIRT
            part = increment[start : start + SKIRT] - ref[target_rows]
            miss_ref[start : start + SKIRT] = ref[weight_rows] * part
        beyond = dot3(side_map, wide_ref[...], (1, 1))
        pieces = []
        for number, ref in enumerate((west_ref, east_ref)):
            tile = slice(number * LANES, (number + 1) * LANES)

            def extended(at):
                start = 4 * SKIRT + at.start
                stop = 4 * SKIRT + at.stop
                last = corner(above_ref[start:stop, tile], below_ref[start:stop, tile])
                return jnp.concatenate([ref[at], last], 1)

            part = beyond[number * SKIRT : (number + 1) * SKIRT]
            pieces.append(extended(weight_rows) * (part - extended(target_rows)))
        beyond = jnp.concatenate(pieces, 0)
        lane_wide = iota((1, width + LANES), 1)
        column = jnp.where(
            lane_wide < width, lane_wide, packed_column(lane_wide - width, level, width)
        )
        back = interpolate(column, lon_cell_up[:cols], lon_share_up[:cols])
        side_back = interpolate(column, lon_cell_up[beside], lon_share_up[beside])
        by_lon = dot3(miss_ref[...], back) + dot3(beyond, side_back, (0, 0))
        residual = dot3(lat_back, by_lon)
        own_ref[level] = residual[:, :width]
        edge_ref[level] = residual[:, width:]


def gradient_kernel(
    width_ref, alpha_ref, perts_ref, above_ref, below_ref, west_ref, east_ref, own_ref, edge_ref, out_ref,
    lon_ref, lat_ref, stack_ref,
):
    height, width = alpha_ref.shape[1], alpha_ref.shape[2]
    ext = height + 2 * HB

    @pl.when(pl.program_id(0) == 0)
    def _():
        for level in range(2):
            spread = width_ref[level].astype(F32)
            source = iota((width, width), 0)
            high, low = split(taps(source - iota((width, width), 1), spread))
            lane = iota((LANES, width), 0)
            edge = taps(packed_column(lane, level, width) - iota((LANES, width), 1), spread)
            for t in range(MEMBERS):
                part_high, part_low = split(jnp.where(packed_member(lane) == t, edge, 0.0))
                lon_ref[level, t, :width, :width] = high
                lon_ref[level, t, :width, width:] = low
                lon_ref[level, t, width:, :width] = part_high
                lon_ref[level, t, width:, width:] = part_low
            source = row_of(iota((height, ext), 1), height)
            high, low = split(taps(source - iota((height, ext), 0), spread))
            lat_ref[level, :, :ext] = high
            lat_ref[level, :, ext : 2 * ext] = low
            lat_ref[level, :, 2 * ext :] = high

    half = iota((ext, LANES), 1) < LANES // 2
    west = west_ref[0].astype(F32)
    east = east_ref[0].astype(F32)

    def stack(value, start, size):
        high, low = split(value)
        stack_ref[:ext, start : start + size] = high
        stack_ref[ext : 2 * ext, start : start + size] = high
        stack_ref[2 * ext :, start : start + size] = low

    for level in range(2):
        cell = jnp.where(half, west, east) if level == 0 else jnp.where(half, east, west)
        stack(cell * edge_ref[level], MEMBERS * width, LANES)
        for t in range(MEMBERS):
            k = 2 * t + level
            field = jnp.concatenate(
                [perts_ref[k].astype(F32), above_ref[k].astype(F32), below_ref[k].astype(F32)], 0
            )
            stack(field * own_ref[level], t * width, width)
        edge_high, edge_low = split(dot(lat_ref[level], stack_ref[:, MEMBERS * width :]))
        for pair in range(MEMBERS // 2):
            base = 2 * pair * width
            wide = dot(lat_ref[level], stack_ref[:, base : base + 2 * width])
            for side in range(2):
                t = 2 * pair + side
                k = 2 * t + level
                high, low = split(wide[:, side * width : (side + 1) * width])
                main = dot(jnp.concatenate([high, edge_high], 1), lon_ref[level, t])
                rest = dot(jnp.concatenate([low, edge_low], 1), lon_ref[level, t, :, :width])
                total = main[:, :width] + main[:, width:] + rest
                out_ref[k] = alpha_ref[k].astype(F32) + total


def ring(axis, periodic):
    count = lax.axis_size(axis)
    forward = [(i, i + 1) for i in range(count - 1)]
    if periodic:
        forward.append((count - 1, 0))
    return forward, [(target, source) for source, target in forward]


def exchange(to_next, to_previous, axis, periodic):
    forward, backward = ring(axis, periodic)
    return lax.ppermute(to_next, axis, forward), lax.ppermute(to_previous, axis, backward)


def vmem(*shape):
    return pl.BlockSpec(shape, lambda s: (0,) * len(shape))


def grouped(*shape):
    return pl.BlockSpec(shape, lambda s: (s,) + (0,) * (len(shape) - 1))


def shaped(shape, dtype=F32):
    return jax.ShapeDtypeStruct(shape, dtype)


def body(
    alpha_fields,
    member_perts,
    band_widths,
    lat_index,
    lat_weight,
    lon_index,
    lon_weight,
    innovation,
    obs_weight,
):
    members, levels, height, width = alpha_fields.shape
    fields = members * levels
    groups = fields // GROUP
    ext = height + 2 * HB
    fine_h, fine_w = innovation.shape[1], innovation.shape[2]
    alpha = alpha_fields.reshape(fields, height, width)
    perts = member_perts.reshape(fields, height, width)
    smem = pl.BlockSpec(memory_space=pltpu.SMEM)
    anywhere = pl.BlockSpec(memory_space=pl.ANY)
    limit = min(60, 16 * (width // LANES)) * 1024 * 1024
    lanes = rounded(width + 2 * HB, LANES)
    tall = rounded(ext + 2 * STRIP, LANES)

    def params(*semantics):
        return pltpu.CompilerParams(dimension_semantics=semantics, vmem_limit_bytes=limit)

    def call(kernel, out_shape, name, flops=10**8, **more):
        return pl.pallas_call(
            kernel,
            out_shape=out_shape,
            compiler_params=params(*(("arbitrary",) if "grid" in more else ())),
            name=name,
            cost_estimate=pl.CostEstimate(flops=flops, bytes_accessed=10**6, transcendentals=0),
            **more,
        )

    edge = shaped((fields, HB, width), BF16)
    to_next, to_previous = call(
        rows_kernel,
        [edge, edge],
        "rows",
        in_specs=[
            pl.BlockSpec((fields, HB, width), lambda s: (0, height // HB - 1, 0)),
            pl.BlockSpec((fields, HB, width), lambda s: (0, 0, 0)),
        ],
        grid=(1,),
        out_specs=[vmem(fields, HB, width)] * 2,
    )(perts, perts)
    above, below = exchange(to_next, to_previous, "gy", False)

    side = shaped((4 * SKIRT + 8, fine_h))
    to_next, to_previous = call(fine_cols_kernel, [side, side], "fine_cols")(
        innovation, obs_weight, lon_index, lon_weight
    )
    fine_west, fine_east = exchange(to_next, to_previous, "gx", True)

    packed = shaped((groups, ext, LANES), BF16)
    to_next, to_previous = call(
        pack_kernel,
        [packed, packed],
        "pack",
        grid=(groups,),
        in_specs=[grouped(GROUP, height, width)] + [grouped(GROUP, HB, width)] * 2,
        out_specs=[grouped(1, ext, LANES)] * 2,
    )(perts, above, below)
    west, east = exchange(to_next, to_previous, "gx", True)

    strip = shaped((8 * SKIRT + 8, fine_w))
    to_next, to_previous, token = call(
        fine_rows_kernel, [strip, strip, shaped((8, LANES))], "fine_rows"
    )(innovation, obs_weight, lat_index, lat_weight, fine_west, fine_east)
    fine_above, fine_below = exchange(to_next, to_previous, "gy", False)

    partial, edge_rows, edge_cols = call(
        local_kernel,
        [
            shaped((2, height, width)),
            shaped((fields, 2 * HB, width)),
            shaped((groups, 2, ext, LANES)),
        ],
        "local",
        flops=10**10,
        grid=(groups,),
        in_specs=[
            smem,
            grouped(GROUP, height, width),
            grouped(GROUP, height, width),
            anywhere,
        ],
        out_specs=[
            vmem(2, height, width),
            grouped(GROUP, 2 * HB, width),
            grouped(1, 2, ext, LANES),
        ],
        scratch_shapes=[
            pltpu.VMEM((2, MEMBERS, 2 * width, width + LANES), BF16),
            pltpu.VMEM((2, ext, 3 * height), BF16),
            pltpu.VMEM((3 * height, MEMBERS * width + LANES), BF16),
        ],
    )(band_widths, alpha, perts, token)

    framed = call(frame_kernel, shaped((2, ext, width + LANES)), "frame")(
        partial, edge_rows, edge_cols, above, below, west, east
    )
    count = lax.axis_size("ma")
    other = lax.ppermute(framed, "ma", [(i, (i + 1) % count) for i in range(count)])
    strip = shaped((2, STRIP, lanes))
    framed, to_next, to_previous = call(
        total_kernel, [shaped((2, ext, lanes)), strip, strip], "total"
    )(framed, other)
    north, south = exchange(to_next, to_previous, "gy", False)
    strip = shaped((2 * STRIP, tall))
    stack, to_next, to_previous = call(
        functools.partial(strips_kernel, width), [shaped((2, tall, lanes)), strip, strip], "strips"
    )(framed, north, south)
    strip_west, strip_east = exchange(to_next, to_previous, "gx", True)

    starts = jnp.stack([lax.axis_index("gy") * height, lax.axis_index("gx") * width])
    lon_total = width * lax.axis_size("gx")
    everything = [pl.BlockSpec(memory_space=pltpu.VMEM)] * 13
    increment, own, edge = call(
        functools.partial(fine_kernel, lon_total),
        [shaped((2, fine_h, fine_w)), shaped((2, ext, width)), shaped((2, ext, LANES))],
        "fine",
        in_specs=[smem] + everything,
        scratch_shapes=[
            pltpu.VMEM((fine_h + LANES, lanes + LANES), F32),
            pltpu.VMEM((fine_h + LANES, fine_w), F32),
        ],
    )(
        starts,
        stack,
        strip_west,
        strip_east,
        innovation,
        obs_weight,
        lat_index,
        lat_weight,
        lon_index,
        lon_weight,
        fine_west,
        fine_east,
        fine_above,
        fine_below,
    )

    gradient = call(
        gradient_kernel,
        shaped((fields, height, width)),
        "gradient",
        grid=(groups,),
        in_specs=[
            smem,
            grouped(GROUP, height, width),
            grouped(GROUP, height, width),
            grouped(GROUP, HB, width),
            grouped(GROUP, HB, width),
            grouped(1, ext, LANES),
            grouped(1, ext, LANES),
            vmem(2, ext, width),
            vmem(2, ext, LANES),
        ],
        out_specs=grouped(GROUP, height, width),
        scratch_shapes=[
            pltpu.VMEM((2, MEMBERS, width + LANES, 2 * width), BF16),
            pltpu.VMEM((2, height, 3 * ext), BF16),
            pltpu.VMEM((3 * ext, MEMBERS * width + LANES), BF16),
        ],
    )(band_widths, alpha, perts, above, below, west, east, own, edge)
    return increment, gradient.reshape(alpha_fields.shape)


def solution(mesh):
    placed = (
        P("ma", None, "gy", "gx"),
        P("ma", None, "gy", "gx"),
        P(),
        P("gy"),
        P("gy"),
        P("gx"),
        P("gx"),
        P(None, "gy", "gx"),
        P(None, "gy", "gx"),
    )
    return jax.shard_map(
        body,
        mesh=mesh,
        in_specs=placed,
        out_specs=(P(None, "gy", "gx"), P("ma", None, "gy", "gx")),
        check_vma=False,
    )
```

```python
import functools

import jax
import jax.numpy as jnp
from jax import lax
from jax.experimental import pallas as pl
from jax.experimental.pallas import tpu as pltpu
from jax.sharding import PartitionSpec as P

HB = 8
GROUP = 16
MEMBERS = 8
SKIRT = 24
STRIP = 24
NOWHERE = -9999
LANES = 128
F32 = jnp.float32
BF16 = jnp.bfloat16


def rounded(size, step):
    return -(-size // step) * step


def iota(shape, axis):
    return lax.broadcasted_iota(jnp.int32, shape, axis)


def split(value):
    high = value.astype(BF16)
    return high, (value - high.astype(F32)).astype(BF16)


def dot(left, right, dims=(1, 0)):
    return lax.dot_general(
        left, right, (((dims[0],), (dims[1],)), ((), ())), preferred_element_type=F32
    )


def dot3(left, right, dims=(1, 0)):
    left_high, left_low = split(left)
    right_high, right_low = split(right)
    total = dot(left_high, right_low, dims) + dot(left_low, right_high, dims)
    return total + dot(left_high, right_high, dims)


def row_of(index, height):
    above = index - height - HB
    return jnp.where(index < height, index, jnp.where(index < height + HB, above, index - HB))


def packed_column(lane, level, width):
    west = (lane < LANES // 2) if level == 0 else (lane >= LANES // 2)
    cell = lane & (HB - 1)
    return jnp.where(west, cell - HB, width + cell)


def packed_member(lane):
    return (lane & (LANES // 2 - 1)) >> 3


def taps(offset, spread):
    lane = iota((8, LANES), 1)
    distance = (lane - HB).astype(F32)
    scale = jnp.full((8, LANES), 1.0, F32) * (0.5 / (spread * spread))
    shape = jnp.where(lane <= 2 * HB, jnp.exp(-(distance * distance) * scale), 0.0)
    norm = lax.rsqrt(jnp.sum(shape * shape, axis=1, keepdims=True))[:1, :1]
    far = offset.astype(F32)
    value = jnp.exp(-(far * far) * scale[:1, :1]) * norm
    return jnp.where(jnp.abs(offset) <= HB, value, 0.0)


def pack_kernel(perts_ref, above_ref, below_ref, east_ref, west_ref):
    rows = east_ref.shape[1]
    width = perts_ref.shape[2]
    lane = iota((rows, LANES), 1)
    east = jnp.zeros((rows, LANES), F32)
    west = jnp.zeros((rows, LANES), F32)
    for k in range(GROUP):
        t, level = k // 2, k % 2
        own = perts_ref[k]
        whole = jnp.concatenate(
            [own.astype(F32), above_ref[k].astype(F32), below_ref[k].astype(F32)], 0
        )
        last = whole[:, width - LANES :]
        first = whole[:, :LANES]
        slot = level * (LANES // 2) + t * HB
        other = (1 - level) * (LANES // 2) + t * HB
        last = pltpu.roll(last, (slot + HB) % LANES, 1)
        first = first if other == 0 else pltpu.roll(first, other, 1)
        east = jnp.where(lane >> 3 == slot // HB, last, east)
        west = jnp.where(lane >> 3 == other // HB, first, west)
    east_ref[0] = east.astype(BF16)
    west_ref[0] = west.astype(BF16)


def local_kernel(
    width_ref, alpha_ref, perts_ref, token_ref, sum_ref, rows_ref, cols_ref, lon_ref, lat_ref, stack_ref
):
    height, width = alpha_ref.shape[1], alpha_ref.shape[2]
    ext = height + 2 * HB

    @pl.when(pl.program_id(0) == 0)
    def _():
        sum_ref[...] = jnp.zeros_like(sum_ref)
        for level in range(2):
            spread = width_ref[level].astype(F32)
            source = iota((width, width), 0)
            high, low = split(taps(source - iota((width, width), 1), spread))
            source = iota((width, LANES), 0)
            lane = iota((width, LANES), 1)
            edge = taps(source - packed_column(lane, level, width), spread)
            for t in range(MEMBERS):
                part_high, part_low = split(jnp.where(packed_member(lane) == t, edge, 0.0))
                lon_ref[level, t, :width, :width] = high
                lon_ref[level, t, width:, :width] = low
                lon_ref[level, t, :width, width:] = part_high
                lon_ref[level, t, width:, width:] = part_low
            target = row_of(iota((ext, height), 0), height)
            high, low = split(taps(target - iota((ext, height), 1), spread))
            lat_ref[level, :, :height] = high
            lat_ref[level, :, height : 2 * height] = low
            lat_ref[level, :, 2 * height :] = high

    for level in range(2):
        packed = jnp.zeros((height, LANES), F32)
        for t in range(MEMBERS):
            field = alpha_ref[2 * t + level]
            both = dot(jnp.concatenate([field, field], 1), lon_ref[level, t])
            high, low = split(both[:, :width])
            stack_ref[:height, t * width : (t + 1) * width] = high
            stack_ref[height : 2 * height, t * width : (t + 1) * width] = high
            stack_ref[2 * height :, t * width : (t + 1) * width] = low
            packed = packed + both[:, width:]
        high, low = split(packed)
        stack_ref[:height, MEMBERS * width :] = high
        stack_ref[height : 2 * height, MEMBERS * width :] = high
        stack_ref[2 * height :, MEMBERS * width :] = low
        total = sum_ref[level]
        for pair in range(MEMBERS // 2):
            base = 2 * pair * width
            wide = dot(lat_ref[level], stack_ref[:, base : base + 2 * width])
            for side in range(2):
                k = 2 * (2 * pair + side) + level
                field = wide[:, side * width : (side + 1) * width]
                total = total + perts_ref[k].astype(F32) * field[:height]
                rows_ref[k] = field[height:]
        sum_ref[level] = total
        cols_ref[0, level] = dot(lat_ref[level], stack_ref[:, MEMBERS * width :])


def stacked_cell(index, size, base):
    cell = row_of(index, size)
    low = index - base
    cell = jnp.where(index < size + 2 * HB, cell, NOWHERE)
    cell = jnp.where((low >= 0) & (low < STRIP), low - 2 * HB, cell)
    return jnp.where((low >= STRIP) & (low < 2 * STRIP), low - STRIP + size - HB, cell)


def interpolate(cell, index, weight):
    near = jnp.where(cell == index, 1.0 - weight, 0.0)
    return near + jnp.where(cell == index + 1, weight, 0.0)


def rows_kernel(perts_ref, next_ref, previous_ref, sems):
    height = perts_ref.shape[1]
    copies = [
        pltpu.make_async_copy(perts_ref.at[:, height - HB :], next_ref, sems.at[0]),
        pltpu.make_async_copy(perts_ref.at[:, :HB], previous_ref, sems.at[1]),
    ]
    for copy in copies:
        copy.start()
    for copy in copies:
        copy.wait()


def table(index, weight):
    size = index.shape[-1]
    row = iota((8, size), 0)
    return jnp.where(
        row == 0, index.astype(F32).reshape(1, size), jnp.where(row == 1, weight.reshape(1, size), 0.0)
    )


def fine_cols_kernel(target_ref, weight_ref, index_ref, share_ref, east_ref, west_ref):
    cols = target_ref.shape[2]
    for a, ref in enumerate((target_ref, weight_ref)):
        for level in range(2):
            start = (2 * a + level) * SKIRT
            east_ref[start : start + SKIRT] = ref[level, :, cols - LANES :].T[LANES - SKIRT :]
            west_ref[start : start + SKIRT] = ref[level, :, :LANES].T[:SKIRT]
    lon = table(index_ref[...], share_ref[...])
    east_ref[4 * SKIRT :, :LANES] = lon[:, cols - LANES :]
    west_ref[4 * SKIRT :, :LANES] = lon[:, :LANES]


def fine_rows_kernel(
    target_ref, weight_ref, index_ref, share_ref, west_ref, east_ref, order_ref, next_ref, previous_ref,
    token_ref,
):
    rows = target_ref.shape[1]
    for a, ref in enumerate((target_ref, weight_ref)):
        for level in range(2):
            start = (2 * a + level) * SKIRT
            next_ref[start : start + SKIRT] = ref[level, rows - SKIRT :]
            previous_ref[start : start + SKIRT] = ref[level, :SKIRT]
    lat = table(index_ref[...], share_ref[...])
    for side, ref in enumerate((west_ref, east_ref)):
        lanes = slice(side * LANES, (side + 1) * LANES)
        next_ref[4 * SKIRT : 8 * SKIRT, lanes] = ref[: 4 * SKIRT, rows - LANES :]
        previous_ref[4 * SKIRT : 8 * SKIRT, lanes] = ref[: 4 * SKIRT, :LANES]
    next_ref[8 * SKIRT :, :LANES] = lat[:, rows - LANES :]
    previous_ref[8 * SKIRT :, :LANES] = lat[:, :LANES]
    token_ref[...] = lat[:, :LANES]


def frame_kernel(
    sum_ref, rows_ref, cols_ref, above_ref, below_ref, west_ref, east_ref, order_ref, after_ref, out_ref
):
    height, width = sum_ref.shape[1], sum_ref.shape[2]
    ext = height + 2 * HB
    groups = west_ref.shape[0]
    half = iota((ext, LANES), 1) < LANES // 2
    for level in range(2):
        edge = jnp.zeros((2 * HB, width), F32)
        packed = jnp.zeros((ext, LANES), F32)
        for group in range(groups):
            for t in range(MEMBERS):
                k = group * GROUP + 2 * t + level
                halo = jnp.concatenate([above_ref[k].astype(F32), below_ref[k].astype(F32)], 0)
                edge = edge + halo * rows_ref[k]
            west = west_ref[group].astype(F32)
            east = east_ref[group].astype(F32)
            cell = jnp.where(half, west, east) if level == 0 else jnp.where(half, east, west)
            packed = packed + cell * cols_ref[group, level]
        column = packed_column(iota((LANES, LANES), 0), level, width)
        slot = iota((LANES, LANES), 1)
        target = jnp.where(slot < HB, slot - HB, jnp.where(slot < 2 * HB, slot - HB + width, NOWHERE))
        gather = (column == target).astype(BF16)
        high, low = split(packed)
        out_ref[level, :height, :width] = sum_ref[level]
        out_ref[level, height:, :width] = edge
        out_ref[level, :, width:] = dot(high, gather) + dot(low, gather)


def total_kernel(mine_ref, other_ref, total_ref, next_ref, previous_ref):
    total = mine_ref[...] + other_ref[...]
    height = total.shape[1] - 2 * HB
    total_ref[...] = total
    next_ref[:, : 2 * HB] = total[:, height - 2 * HB : height]
    next_ref[:, 2 * HB :] = total[:, height + HB :]
    previous_ref[:, :HB] = total[:, height : height + HB]
    previous_ref[:, HB:] = total[:, : 2 * HB]


def strips_kernel(width, total_ref, above_ref, below_ref, stack_ref, east_ref, west_ref):
    ext, lanes = total_ref.shape[1], total_ref.shape[2]
    rows = stack_ref.shape[1]
    column = stacked_cell(iota((STRIP, lanes), 1), width, lanes)
    number = iota((STRIP, lanes), 0)
    pick_east = (column == number + width - 2 * HB).astype(BF16)
    pick_west = (column == number - HB).astype(BF16)
    for level in range(2):
        stack_ref[level, :ext] = total_ref[level]
        stack_ref[level, ext : ext + STRIP] = above_ref[level]
        stack_ref[level, ext + STRIP : ext + 2 * STRIP] = below_ref[level]
        stack_ref[level, ext + 2 * STRIP :] = jnp.zeros((rows - ext - 2 * STRIP, lanes), F32)
        high, low = split(stack_ref[level])
        part = slice(level * STRIP, (level + 1) * STRIP)
        east_ref[part] = dot(pick_east, high, (1, 1)) + dot(pick_east, low, (1, 1))
        west_ref[part] = dot(pick_west, high, (1, 1)) + dot(pick_west, low, (1, 1))


def fine_kernel(
    lon_total,
    stack_ref,
    strip_west_ref,
    strip_east_ref,
    target_ref,
    weight_ref,
    lat_index_ref,
    lat_share_ref,
    lon_index_ref,
    lon_share_ref,
    west_ref,
    east_ref,
    above_ref,
    below_ref,
    inc_ref,
    own_ref,
    edge_ref,
    wide_ref,
    miss_ref,
):
    ext, width = own_ref.shape[1], own_ref.shape[2]
    height = ext - 2 * HB
    rows, cols = target_ref.shape[1], target_ref.shape[2]
    lanes = stack_ref.shape[2]
    span = rows + LANES
    lane = iota((8, LANES), 1)
    first = iota((8, LANES), 0) == 0

    def side(low, high):
        low = pltpu.roll(low, SKIRT, 1)
        high = pltpu.roll(high, SKIRT, 1)
        blank = jnp.where(first, 1.0e6, 0.0)
        return jnp.where(lane < SKIRT, low, jnp.where(lane < 2 * SKIRT, high, blank))

    def corner(low, high):
        spot = iota(low.shape, 1)
        low = pltpu.roll(low, SKIRT, 1)
        high = pltpu.roll(high, SKIRT, 1)
        return jnp.where(spot < SKIRT, low, jnp.where(spot < 2 * SKIRT, high, 0.0))

    lat_side = side(above_ref[8 * SKIRT :, :LANES], below_ref[8 * SKIRT :, :LANES])
    lat = jnp.concatenate([table(lat_index_ref[...], lat_share_ref[...]), lat_side], 1)
    lon_side = side(west_ref[4 * SKIRT :, :LANES], east_ref[4 * SKIRT :, :LANES])
    lon = jnp.concatenate([table(lon_index_ref[...], lon_share_ref[...]), lon_side], 1)
    lat_cell = lat[0:1].astype(jnp.int32) - lax.axis_index("gy") * height
    lat_share = lat[1:2]
    lon_cell = lon[0:1].astype(jnp.int32) - lax.axis_index("gx") * width
    lon_cell = jnp.where(lon_cell < -(lon_total // 2), lon_cell + lon_total, lon_cell)
    wrap = (lon_cell >= lon_total // 2) & (lon_cell < lon_total)
    lon_cell = jnp.where(wrap, lon_cell - lon_total, lon_cell)
    lon_share = lon[1:2]
    upright = jnp.concatenate([lat_cell.astype(F32), lat_share, jnp.zeros((6, span), F32)], 0).T
    lat_cell_up, lat_share_up = upright[:, 0:1].astype(jnp.int32), upright[:, 1:2]
    upright = jnp.concatenate(
        [lon_cell.astype(F32), lon_share, jnp.zeros((6, cols + LANES), F32)], 0
    ).T
    lon_cell_up, lon_share_up = upright[:, 0:1].astype(jnp.int32), upright[:, 1:2]
    beside = slice(cols, cols + 2 * SKIRT)

    tall = stack_ref.shape[1]
    lat_map = interpolate(
        stacked_cell(iota((span, tall), 1), height, ext), lat_cell_up, lat_share_up
    )
    broad = lanes + LANES
    lon_map = interpolate(
        stacked_cell(iota((broad, cols), 0), width, lanes), lon_cell[:, :cols], lon_share[:, :cols]
    )
    side_map = interpolate(
        stacked_cell(iota((2 * SKIRT, broad), 1), width, lanes),
        lon_cell_up[beside],
        lon_share_up[beside],
    )
    lat_back = interpolate(row_of(iota((ext, span), 0), height), lat_cell, lat_share)
    lat_high, lat_low = split(lat_map)
    wide_ref[:, lanes:] = jnp.zeros((span, LANES), F32)
    miss_ref[rows + 2 * SKIRT :] = jnp.zeros((span - rows - 2 * SKIRT, cols), F32)

    for level in range(2):
        wide_ref[:, :lanes] = dot3(lat_map, stack_ref[level])
        part = slice(level * STRIP, (level + 1) * STRIP)
        strips = jnp.concatenate([strip_west_ref[part], strip_east_ref[part]], 0)
        wide_ref[:, lanes : lanes + 2 * STRIP] = dot3(lat_map, strips, (1, 1))
        increment = dot3(wide_ref[...], lon_map)
        inc_ref[level] = increment[:rows]
        miss_ref[:rows] = weight_ref[level] * (increment[:rows] - target_ref[level])
        target_rows = slice(level * SKIRT, (level + 1) * SKIRT)
        weight_rows = slice((2 + level) * SKIRT, (3 + level) * SKIRT)
        for number, ref in enumerate((above_ref, below_ref)):
            start = rows + number * SKIRT
            part = increment[start : start + SKIRT] - ref[target_rows]
            miss_ref[start : start + SKIRT] = ref[weight_rows] * part
        beyond = dot3(side_map, wide_ref[...], (1, 1))
        pieces = []
        for number, ref in enumerate((west_ref, east_ref)):
            tile = slice(number * LANES, (number + 1) * LANES)

            def extended(at):
                start = 4 * SKIRT + at.start
                stop = 4 * SKIRT + at.stop
                last = corner(above_ref[start:stop, tile], below_ref[start:stop, tile])
                return jnp.concatenate([ref[at], last], 1)

            part = beyond[number * SKIRT : (number + 1) * SKIRT]
            pieces.append(extended(weight_rows) * (part - extended(target_rows)))
        beyond = jnp.concatenate(pieces, 0)
        lane_wide = iota((1, width + LANES), 1)
        column = jnp.where(
            lane_wide < width, lane_wide, packed_column(lane_wide - width, level, width)
        )
        back = interpolate(column, lon_cell_up[:cols], lon_share_up[:cols])
        side_back = interpolate(column, lon_cell_up[beside], lon_share_up[beside])
        by_lon = dot3(miss_ref[...], back) + dot3(beyond, side_back, (0, 0))
        residual = dot3(lat_back, by_lon)
        own_ref[level] = residual[:, :width]
        edge_ref[level] = residual[:, width:]


def gradient_kernel(
    width_ref, alpha_ref, perts_ref, above_ref, below_ref, west_ref, east_ref, own_ref, edge_ref, out_ref,
    lon_ref, lat_ref, stack_ref,
):
    height, width = alpha_ref.shape[1], alpha_ref.shape[2]
    ext = height + 2 * HB

    @pl.when(pl.program_id(0) == 0)
    def _():
        for level in range(2):
            spread = width_ref[level].astype(F32)
            source = iota((width, width), 0)
            high, low = split(taps(source - iota((width, width), 1), spread))
            lane = iota((LANES, width), 0)
            edge = taps(packed_column(lane, level, width) - iota((LANES, width), 1), spread)
            for t in range(MEMBERS):
                part_high, part_low = split(jnp.where(packed_member(lane) == t, edge, 0.0))
                lon_ref[level, t, :width, :width] = high
                lon_ref[level, t, :width, width:] = low
                lon_ref[level, t, width:, :width] = part_high
                lon_ref[level, t, width:, width:] = part_low
            source = row_of(iota((height, ext), 1), height)
            high, low = split(taps(source - iota((height, ext), 0), spread))
            lat_ref[level, :, :ext] = high
            lat_ref[level, :, ext : 2 * ext] = low
            lat_ref[level, :, 2 * ext :] = high

    half = iota((ext, LANES), 1) < LANES // 2

    def stacked(value):
        high, low = split(value)
        return jnp.concatenate([high, high, low], 0)

    for level in range(2):
        west = west_ref[0].astype(F32)
        east = east_ref[0].astype(F32)
        cell = jnp.where(half, west, east) if level == 0 else jnp.where(half, east, west)
        side = dot(lat_ref[level], stacked(cell * edge_ref[level]))
        side = jnp.concatenate(split(side), 0)
        stack_ref[...] = side
        own = own_ref[level]

        def pair(p, carry):
            columns = []
            for number in range(2):
                k = 4 * p + 2 * number + level
                field = jnp.concatenate(
                    [perts_ref[k].astype(F32), above_ref[k].astype(F32), below_ref[k].astype(F32)], 0
                )
                columns.append(stacked(field * own_ref[level]))
            wide = dot(lat_ref[level], jnp.concatenate(columns, 1))
            for number in range(2):
                t = 2 * p + number
                k = 4 * p + 2 * number + level
                parts = jnp.concatenate(split(wide[:, number * width : (number + 1) * width]), 0)
                both = dot(jnp.concatenate([parts, stack_ref[...]], 1), lon_ref[level, t])
                total = both[:height, :width] + both[:height, width:] + both[height:, :width]
                out_ref[k] = alpha_ref[k].astype(F32) + total
            return carry

        lax.fori_loop(0, MEMBERS // 2, pair, 0, unroll=4)


def GRAD_SCRATCH(height, width):
    ext = height + 2 * HB
    return [
        pltpu.VMEM((2, MEMBERS, width + LANES, 2 * width), BF16),
        pltpu.VMEM((2, height, 3 * ext), BF16),
        pltpu.VMEM((2 * height, LANES), BF16),
    ]


def ring(axis, periodic):
    count = lax.axis_size(axis)
    forward = [(i, i + 1) for i in range(count - 1)]
    if periodic:
        forward.append((count - 1, 0))
    return forward, [(target, source) for source, target in forward]


def exchange(to_next, to_previous, axis, periodic):
    forward, backward = ring(axis, periodic)
    return lax.ppermute(to_next, axis, forward), lax.ppermute(to_previous, axis, backward)


def vmem(*shape):
    return pl.BlockSpec(shape, lambda s: (0,) * len(shape))


def grouped(*shape):
    return pl.BlockSpec(shape, lambda s: (s,) + (0,) * (len(shape) - 1))


def shaped(shape, dtype=F32):
    return jax.ShapeDtypeStruct(shape, dtype)


def body(
    alpha_fields,
    member_perts,
    band_widths,
    lat_index,
    lat_weight,
    lon_index,
    lon_weight,
    innovation,
    obs_weight,
):
    members, levels, height, width = alpha_fields.shape
    fields = members * levels
    groups = fields // GROUP
    ext = height + 2 * HB
    fine_h, fine_w = innovation.shape[1], innovation.shape[2]
    alpha = alpha_fields.reshape(fields, height, width)
    perts = member_perts.reshape(fields, height, width)
    smem = pl.BlockSpec(memory_space=pltpu.SMEM)
    anywhere = pl.BlockSpec(memory_space=pl.ANY)
    scale = width // LANES
    lanes = rounded(width + 2 * HB, LANES)
    tall = rounded(ext + 2 * STRIP, LANES)

    def call(kernel, out_shape, name, flops=10**8, grant=4, **more):
        semantics = ("arbitrary",) if "grid" in more else ()
        return pl.pallas_call(
            kernel,
            out_shape=out_shape,
            compiler_params=pltpu.CompilerParams(
                dimension_semantics=semantics, vmem_limit_bytes=min(60, grant * scale) * 1024 * 1024
            ),
            name=name,
            cost_estimate=pl.CostEstimate(flops=flops, bytes_accessed=10**6, transcendentals=0),
            **more,
        )

    edge = shaped((fields, HB, width), BF16)
    to_next, to_previous = call(
        rows_kernel,
        [edge, edge],
        "rows",
        in_specs=[pl.BlockSpec(memory_space=pltpu.HBM)],
        out_specs=[pl.BlockSpec(memory_space=pltpu.VMEM)] * 2,
        scratch_shapes=[pltpu.SemaphoreType.DMA((2,))],
    )(perts)
    above, below = exchange(to_next, to_previous, "gy", False)

    side = shaped((4 * SKIRT + 8, fine_h))
    to_next, to_previous = call(fine_cols_kernel, [side, side], "fine_cols")(
        innovation, obs_weight, lon_index, lon_weight
    )
    fine_west, fine_east = exchange(to_next, to_previous, "gx", True)

    packed = shaped((groups, ext, LANES), BF16)
    to_next, to_previous = call(
        pack_kernel,
        [packed, packed],
        "pack",
        grant=8,
        grid=(groups,),
        in_specs=[grouped(GROUP, height, width)] + [grouped(GROUP, HB, width)] * 2,
        out_specs=[grouped(1, ext, LANES)] * 2,
    )(perts, above, below)
    west, east = exchange(to_next, to_previous, "gx", True)

    strip = shaped((8 * SKIRT + 8, fine_w))
    whole = pl.BlockSpec(memory_space=pltpu.VMEM)
    to_next, to_previous, token = call(
        fine_rows_kernel,
        [strip, strip, shaped((8, LANES))],
        "fine_rows",
        in_specs=[whole] * 6 + [anywhere],
    )(innovation, obs_weight, lat_index, lat_weight, fine_west, fine_east, to_next)
    fine_above, fine_below = exchange(to_next, to_previous, "gy", False)

    partial, edge_rows, edge_cols = call(
        local_kernel,
        [
            shaped((2, height, width)),
            shaped((fields, 2 * HB, width)),
            shaped((groups, 2, ext, LANES)),
        ],
        "local",
        flops=10**10,
        grant=16,
        grid=(groups,),
        in_specs=[
            smem,
            grouped(GROUP, height, width),
            grouped(GROUP, height, width),
            anywhere,
        ],
        out_specs=[
            vmem(2, height, width),
            grouped(GROUP, 2 * HB, width),
            grouped(1, 2, ext, LANES),
        ],
        scratch_shapes=[
            pltpu.VMEM((2, MEMBERS, 2 * width, width + LANES), BF16),
            pltpu.VMEM((2, ext, 3 * height), BF16),
            pltpu.VMEM((3 * height, MEMBERS * width + LANES), BF16),
        ],
    )(band_widths, alpha, perts, token)

    framed = call(
        frame_kernel,
        shaped((2, ext, width + LANES)),
        "frame",
        in_specs=[whole] * 7 + [anywhere] * 2,
    )(partial, edge_rows, edge_cols, above, below, west, east, fine_above, fine_below)
    count = lax.axis_size("ma")
    other = lax.ppermute(framed, "ma", [(i, (i + 1) % count) for i in range(count)])
    strip = shaped((2, STRIP, lanes))
    framed, to_next, to_previous = call(
        total_kernel, [shaped((2, ext, lanes)), strip, strip], "total"
    )(framed, other)
    north, south = exchange(to_next, to_previous, "gy", False)
    strip = shaped((2 * STRIP, tall))
    stack, to_next, to_previous = call(
        functools.partial(strips_kernel, width), [shaped((2, tall, lanes)), strip, strip], "strips"
    )(framed, north, south)
    strip_west, strip_east = exchange(to_next, to_previous, "gx", True)

    lon_total = width * lax.axis_size("gx")
    everything = [pl.BlockSpec(memory_space=pltpu.VMEM)] * 13
    increment, own, edge = call(
        functools.partial(fine_kernel, lon_total),
        [shaped((2, fine_h, fine_w)), shaped((2, ext, width)), shaped((2, ext, LANES))],
        "fine",
        grant=16,
        in_specs=everything,
        scratch_shapes=[
            pltpu.VMEM((fine_h + LANES, lanes + LANES), F32),
            pltpu.VMEM((fine_h + LANES, fine_w), F32),
        ],
    )(
        stack,
        strip_west,
        strip_east,
        innovation,
        obs_weight,
        lat_index,
        lat_weight,
        lon_index,
        lon_weight,
        fine_west,
        fine_east,
        fine_above,
        fine_below,
    )

    gradient = call(
        gradient_kernel,
        shaped((fields, height, width)),
        "gradient",
        grant=16,
        grid=(groups,),
        in_specs=[
            smem,
            grouped(GROUP, height, width),
            grouped(GROUP, height, width),
            grouped(GROUP, HB, width),
            grouped(GROUP, HB, width),
            grouped(1, ext, LANES),
            grouped(1, ext, LANES),
            vmem(2, ext, width),
            vmem(2, ext, LANES),
        ],
        out_specs=grouped(GROUP, height, width),
        scratch_shapes=GRAD_SCRATCH(height, width),
    )(band_widths, alpha, perts, above, below, west, east, own, edge)
    return increment, gradient.reshape(alpha_fields.shape)


def solution(mesh):
    placed = (
        P("ma", None, "gy", "gx"),
        P("ma", None, "gy", "gx"),
        P(),
        P("gy"),
        P("gy"),
        P("gx"),
        P("gx"),
        P(None, "gy", "gx"),
        P(None, "gy", "gx"),
    )
    return jax.shard_map(
        body,
        mesh=mesh,
        in_specs=placed,
        out_specs=(P(None, "gy", "gx"), P("ma", None, "gy", "gx")),
        check_vma=False,
    )
```

```python
import functools

import jax
import jax.numpy as jnp
from jax import lax
from jax.experimental import pallas as pl
from jax.experimental.pallas import tpu as pltpu
from jax.sharding import PartitionSpec as P

HB = 8
GROUP = 16
MEMBERS = 8
SKIRT = 24
STRIP = 24
NOWHERE = -9999
LANES = 128
F32 = jnp.float32
BF16 = jnp.bfloat16


def rounded(size, step):
    return -(-size // step) * step


def iota(shape, axis):
    return lax.broadcasted_iota(jnp.int32, shape, axis)


def split(value):
    high = value.astype(BF16)
    return high, (value - high.astype(F32)).astype(BF16)


def dot(left, right, dims=(1, 0)):
    return lax.dot_general(
        left, right, (((dims[0],), (dims[1],)), ((), ())), preferred_element_type=F32
    )


def dot3(left, right, dims=(1, 0)):
    left_high, left_low = split(left)
    right_high, right_low = split(right)
    total = dot(left_high, right_low, dims) + dot(left_low, right_high, dims)
    return total + dot(left_high, right_high, dims)


def row_of(index, height):
    above = index - height - HB
    return jnp.where(index < height, index, jnp.where(index < height + HB, above, index - HB))


def packed_column(lane, level, width):
    west = (lane < LANES // 2) if level == 0 else (lane >= LANES // 2)
    cell = lane & (HB - 1)
    return jnp.where(west, cell - HB, width + cell)


def packed_member(lane):
    return (lane & (LANES // 2 - 1)) >> 3


def taps(offset, spread):
    lane = iota((8, LANES), 1)
    distance = (lane - HB).astype(F32)
    scale = jnp.full((8, LANES), 1.0, F32) * (0.5 / (spread * spread))
    shape = jnp.where(lane <= 2 * HB, jnp.exp(-(distance * distance) * scale), 0.0)
    norm = lax.rsqrt(jnp.sum(shape * shape, axis=1, keepdims=True))[:1, :1]
    far = offset.astype(F32)
    value = jnp.exp(-(far * far) * scale[:1, :1]) * norm
    return jnp.where(jnp.abs(offset) <= HB, value, 0.0)


def pack_kernel(perts_ref, above_ref, below_ref, east_ref, west_ref):
    rows = east_ref.shape[1]
    width = perts_ref.shape[2]
    lane = iota((rows, LANES), 1)
    east = jnp.zeros((rows, LANES), F32)
    west = jnp.zeros((rows, LANES), F32)
    for k in range(GROUP):
        t, level = k // 2, k % 2
        own = perts_ref[k]
        whole = jnp.concatenate(
            [own.astype(F32), above_ref[k].astype(F32), below_ref[k].astype(F32)], 0
        )
        last = whole[:, width - LANES :]
        first = whole[:, :LANES]
        slot = level * (LANES // 2) + t * HB
        other = (1 - level) * (LANES // 2) + t * HB
        last = pltpu.roll(last, (slot + HB) % LANES, 1)
        first = first if other == 0 else pltpu.roll(first, other, 1)
        east = jnp.where(lane >> 3 == slot // HB, last, east)
        west = jnp.where(lane >> 3 == other // HB, first, west)
    east_ref[0] = east.astype(BF16)
    west_ref[0] = west.astype(BF16)


def local_kernel(
    width_ref, alpha_ref, perts_ref, token_ref, sum_ref, rows_ref, cols_ref, lon_ref, lat_ref, stack_ref
):
    height, width = alpha_ref.shape[1], alpha_ref.shape[2]
    ext = height + 2 * HB

    @pl.when(pl.program_id(0) == 0)
    def _():
        sum_ref[...] = jnp.zeros_like(sum_ref)
        for level in range(2):
            spread = width_ref[level].astype(F32)
            source = iota((width, width), 0)
            high, low = split(taps(source - iota((width, width), 1), spread))
            source = iota((width, LANES), 0)
            lane = iota((width, LANES), 1)
            edge = taps(source - packed_column(lane, level, width), spread)
            for t in range(MEMBERS):
                part_high, part_low = split(jnp.where(packed_member(lane) == t, edge, 0.0))
                lon_ref[level, t, :width, :width] = high
                lon_ref[level, t, width:, :width] = low
                lon_ref[level, t, :width, width:] = part_high
                lon_ref[level, t, width:, width:] = part_low
            target = row_of(iota((ext, height), 0), height)
            high, low = split(taps(target - iota((ext, height), 1), spread))
            lat_ref[level, :, :height] = high
            lat_ref[level, :, height : 2 * height] = low
            lat_ref[level, :, 2 * height :] = high

    def put(level, start, value):
        high, low = split(value)
        stop = start + value.shape[1]
        stack_ref[level, :height, start:stop] = high
        stack_ref[level, height : 2 * height, start:stop] = high
        stack_ref[level, 2 * height :, start:stop] = low

    for level in range(2):
        packed = jnp.zeros((height, LANES), F32)
        for t in range(MEMBERS):
            field = alpha_ref[2 * t + level]
            both = dot(jnp.concatenate([field, field], 1), lon_ref[level, t])
            put(level, t * width, both[:, :width])
            packed = packed + both[:, width:]
        put(level, MEMBERS * width, packed)
    for level in range(2):
        total = sum_ref[level]
        for pair in range(MEMBERS // 2):
            base = 2 * pair * width
            wide = dot(lat_ref[level], stack_ref[level, :, base : base + 2 * width])
            for side in range(2):
                k = 2 * (2 * pair + side) + level
                field = wide[:, side * width : (side + 1) * width]
                total = total + perts_ref[k].astype(F32) * field[:height]
                rows_ref[k] = field[height:]
        sum_ref[level] = total
        cols_ref[0, level] = dot(lat_ref[level], stack_ref[level, :, MEMBERS * width :])


def stacked_cell(index, size, base):
    cell = row_of(index, size)
    low = index - base
    cell = jnp.where(index < size + 2 * HB, cell, NOWHERE)
    cell = jnp.where((low >= 0) & (low < STRIP), low - 2 * HB, cell)
    return jnp.where((low >= STRIP) & (low < 2 * STRIP), low - STRIP + size - HB, cell)


def interpolate(cell, index, weight):
    near = jnp.where(cell == index, 1.0 - weight, 0.0)
    return near + jnp.where(cell == index + 1, weight, 0.0)


def seal(axis, next_ref, previous_ref):
    place = lax.axis_index(axis)

    @pl.when(place == lax.axis_size(axis) - 1)
    def _():
        next_ref[...] = jnp.zeros_like(next_ref)

    @pl.when(place == 0)
    def _():
        previous_ref[...] = jnp.zeros_like(previous_ref)


def rows_kernel(perts_ref, next_ref, previous_ref, sems):
    height = perts_ref.shape[1]
    copies = [
        pltpu.make_async_copy(perts_ref.at[:, height - HB :], next_ref, sems.at[0]),
        pltpu.make_async_copy(perts_ref.at[:, :HB], previous_ref, sems.at[1]),
    ]
    for copy in copies:
        copy.start()
    for copy in copies:
        copy.wait()
    seal("gy", next_ref, previous_ref)


def table(index, weight):
    size = index.shape[-1]
    row = iota((8, size), 0)
    return jnp.where(
        row == 0, index.astype(F32).reshape(1, size), jnp.where(row == 1, weight.reshape(1, size), 0.0)
    )


def fine_cols_kernel(target_ref, weight_ref, index_ref, share_ref, east_ref, west_ref):
    cols = target_ref.shape[2]
    for a, ref in enumerate((target_ref, weight_ref)):
        for level in range(2):
            start = (2 * a + level) * SKIRT
            east_ref[start : start + SKIRT] = ref[level, :, cols - LANES :].T[LANES - SKIRT :]
            west_ref[start : start + SKIRT] = ref[level, :, :LANES].T[:SKIRT]
    lon = table(index_ref[...], share_ref[...])
    east_ref[4 * SKIRT :, :LANES] = lon[:, cols - LANES :]
    west_ref[4 * SKIRT :, :LANES] = lon[:, :LANES]


def fine_rows_kernel(
    target_ref, weight_ref, index_ref, share_ref, west_ref, east_ref, order_ref, next_ref, previous_ref,
    token_ref,
):
    rows = target_ref.shape[1]
    for a, ref in enumerate((target_ref, weight_ref)):
        for level in range(2):
            start = (2 * a + level) * SKIRT
            next_ref[start : start + SKIRT] = ref[level, rows - SKIRT :]
            previous_ref[start : start + SKIRT] = ref[level, :SKIRT]
    lat = table(index_ref[...], share_ref[...])
    for side, ref in enumerate((west_ref, east_ref)):
        lanes = slice(side * LANES, (side + 1) * LANES)
        next_ref[4 * SKIRT : 8 * SKIRT, lanes] = ref[: 4 * SKIRT, rows - LANES :]
        previous_ref[4 * SKIRT : 8 * SKIRT, lanes] = ref[: 4 * SKIRT, :LANES]
    next_ref[8 * SKIRT :, :LANES] = lat[:, rows - LANES :]
    previous_ref[8 * SKIRT :, :LANES] = lat[:, :LANES]
    token_ref[...] = lat[:, :LANES]
    seal("gy", next_ref, previous_ref)


def frame_kernel(
    sum_ref, rows_ref, cols_ref, above_ref, below_ref, west_ref, east_ref, out_ref
):
    height, width = sum_ref.shape[1], sum_ref.shape[2]
    ext = height + 2 * HB
    groups = west_ref.shape[0]
    half = iota((ext, LANES), 1) < LANES // 2
    for level in range(2):
        edge = jnp.zeros((2 * HB, width), F32)
        packed = jnp.zeros((ext, LANES), F32)
        for group in range(groups):
            for t in range(MEMBERS):
                k = group * GROUP + 2 * t + level
                halo = jnp.concatenate([above_ref[k].astype(F32), below_ref[k].astype(F32)], 0)
                edge = edge + halo * rows_ref[k]
            west = west_ref[group].astype(F32)
            east = east_ref[group].astype(F32)
            cell = jnp.where(half, west, east) if level == 0 else jnp.where(half, east, west)
            packed = packed + cell * cols_ref[group, level]
        column = packed_column(iota((LANES, LANES), 0), level, width)
        slot = iota((LANES, LANES), 1)
        target = jnp.where(slot < HB, slot - HB, jnp.where(slot < 2 * HB, slot - HB + width, NOWHERE))
        gather = (column == target).astype(BF16)
        high, low = split(packed)
        out_ref[level, :height, :width] = sum_ref[level]
        out_ref[level, height:, :width] = edge
        out_ref[level, :, width:] = dot(high, gather) + dot(low, gather)


def total_kernel(mine_ref, other_ref, total_ref, next_ref, previous_ref):
    total = mine_ref[...] + other_ref[...]
    height = total.shape[1] - 2 * HB
    total_ref[...] = total
    next_ref[:, : 2 * HB] = total[:, height - 2 * HB : height]
    next_ref[:, 2 * HB :] = total[:, height + HB :]
    previous_ref[:, :HB] = total[:, height : height + HB]
    previous_ref[:, HB:] = total[:, : 2 * HB]
    seal("gy", next_ref, previous_ref)


def strips_kernel(width, total_ref, above_ref, below_ref, stack_ref, east_ref, west_ref):
    ext, lanes = total_ref.shape[1], total_ref.shape[2]
    rows = stack_ref.shape[1]
    column = stacked_cell(iota((STRIP, lanes), 1), width, lanes)
    number = iota((STRIP, lanes), 0)
    pick_east = (column == number + width - 2 * HB).astype(BF16)
    pick_west = (column == number - HB).astype(BF16)
    for level in range(2):
        stack_ref[level, :ext] = total_ref[level]
        stack_ref[level, ext : ext + STRIP] = above_ref[level]
        stack_ref[level, ext + STRIP : ext + 2 * STRIP] = below_ref[level]
        stack_ref[level, ext + 2 * STRIP :] = jnp.zeros((rows - ext - 2 * STRIP, lanes), F32)
        high, low = split(stack_ref[level])
        part = slice(level * STRIP, (level + 1) * STRIP)
        east_ref[part] = dot(pick_east, high, (1, 1)) + dot(pick_east, low, (1, 1))
        west_ref[part] = dot(pick_west, high, (1, 1)) + dot(pick_west, low, (1, 1))


def fine_kernel(
    lon_total,
    stack_ref,
    strip_west_ref,
    strip_east_ref,
    target_ref,
    weight_ref,
    lat_index_ref,
    lat_share_ref,
    lon_index_ref,
    lon_share_ref,
    west_ref,
    east_ref,
    above_ref,
    below_ref,
    inc_ref,
    own_ref,
    edge_ref,
    wide_ref,
    miss_ref,
):
    ext, width = own_ref.shape[1], own_ref.shape[2]
    height = ext - 2 * HB
    rows, cols = target_ref.shape[1], target_ref.shape[2]
    lanes = stack_ref.shape[2]
    span = rows + LANES
    lane = iota((8, LANES), 1)
    first = iota((8, LANES), 0) == 0

    def side(low, high):
        low = pltpu.roll(low, SKIRT, 1)
        high = pltpu.roll(high, SKIRT, 1)
        blank = jnp.where(first, 1.0e6, 0.0)
        return jnp.where(lane < SKIRT, low, jnp.where(lane < 2 * SKIRT, high, blank))

    def corner(low, high):
        spot = iota(low.shape, 1)
        low = pltpu.roll(low, SKIRT, 1)
        high = pltpu.roll(high, SKIRT, 1)
        return jnp.where(spot < SKIRT, low, jnp.where(spot < 2 * SKIRT, high, 0.0))

    lat_side = side(above_ref[8 * SKIRT :, :LANES], below_ref[8 * SKIRT :, :LANES])
    lat = jnp.concatenate([table(lat_index_ref[...], lat_share_ref[...]), lat_side], 1)
    lon_side = side(west_ref[4 * SKIRT :, :LANES], east_ref[4 * SKIRT :, :LANES])
    lon = jnp.concatenate([table(lon_index_ref[...], lon_share_ref[...]), lon_side], 1)
    lat_cell = lat[0:1].astype(jnp.int32) - lax.axis_index("gy") * height
    lat_share = lat[1:2]
    lon_cell = lon[0:1].astype(jnp.int32) - lax.axis_index("gx") * width
    lon_cell = jnp.where(lon_cell < -(lon_total // 2), lon_cell + lon_total, lon_cell)
    wrap = (lon_cell >= lon_total // 2) & (lon_cell < lon_total)
    lon_cell = jnp.where(wrap, lon_cell - lon_total, lon_cell)
    lon_share = lon[1:2]
    upright = jnp.concatenate([lat_cell.astype(F32), lat_share, jnp.zeros((6, span), F32)], 0).T
    lat_cell_up, lat_share_up = upright[:, 0:1].astype(jnp.int32), upright[:, 1:2]
    upright = jnp.concatenate(
        [lon_cell.astype(F32), lon_share, jnp.zeros((6, cols + LANES), F32)], 0
    ).T
    lon_cell_up, lon_share_up = upright[:, 0:1].astype(jnp.int32), upright[:, 1:2]
    beside = slice(cols, cols + 2 * SKIRT)

    tall = stack_ref.shape[1]
    lat_map = interpolate(
        stacked_cell(iota((span, tall), 1), height, ext), lat_cell_up, lat_share_up
    )
    broad = lanes + LANES
    lon_map = interpolate(
        stacked_cell(iota((broad, cols), 0), width, lanes), lon_cell[:, :cols], lon_share[:, :cols]
    )
    side_map = interpolate(
        stacked_cell(iota((2 * SKIRT, broad), 1), width, lanes),
        lon_cell_up[beside],
        lon_share_up[beside],
    )
    lat_back = interpolate(row_of(iota((ext, span), 0), height), lat_cell, lat_share)
    lat_high, lat_low = split(lat_map)
    wide_ref[:, lanes:] = jnp.zeros((span, LANES), F32)
    miss_ref[rows + 2 * SKIRT :] = jnp.zeros((span - rows - 2 * SKIRT, cols), F32)

    for level in range(2):
        wide_ref[:, :lanes] = dot3(lat_map, stack_ref[level])
        part = slice(level * STRIP, (level + 1) * STRIP)
        strips = jnp.concatenate([strip_west_ref[part], strip_east_ref[part]], 0)
        wide_ref[:, lanes : lanes + 2 * STRIP] = dot3(lat_map, strips, (1, 1))
        increment = dot3(wide_ref[...], lon_map)
        inc_ref[level] = increment[:rows]
        miss_ref[:rows] = weight_ref[level] * (increment[:rows] - target_ref[level])
        target_rows = slice(level * SKIRT, (level + 1) * SKIRT)
        weight_rows = slice((2 + level) * SKIRT, (3 + level) * SKIRT)
        for number, ref in enumerate((above_ref, below_ref)):
            start = rows + number * SKIRT
            part = increment[start : start + SKIRT] - ref[target_rows]
            miss_ref[start : start + SKIRT] = ref[weight_rows] * part
        beyond = dot3(side_map, wide_ref[...], (1, 1))
        pieces = []
        for number, ref in enumerate((west_ref, east_ref)):
            tile = slice(number * LANES, (number + 1) * LANES)

            def extended(at):
                start = 4 * SKIRT + at.start
                stop = 4 * SKIRT + at.stop
                last = corner(above_ref[start:stop, tile], below_ref[start:stop, tile])
                return jnp.concatenate([ref[at], last], 1)

            part = beyond[number * SKIRT : (number + 1) * SKIRT]
            pieces.append(extended(weight_rows) * (part - extended(target_rows)))
        beyond = jnp.concatenate(pieces, 0)
        lane_wide = iota((1, width + LANES), 1)
        column = jnp.where(
            lane_wide < width, lane_wide, packed_column(lane_wide - width, level, width)
        )
        back = interpolate(column, lon_cell_up[:cols], lon_share_up[:cols])
        side_back = interpolate(column, lon_cell_up[beside], lon_share_up[beside])
        by_lon = dot3(miss_ref[...], back) + dot3(beyond, side_back, (0, 0))
        residual = dot3(lat_back, by_lon)
        own_ref[level] = residual[:, :width]
        edge_ref[level] = residual[:, width:]


def gradient_kernel(
    width_ref, alpha_ref, perts_ref, above_ref, below_ref, west_ref, east_ref, own_ref, edge_ref, out_ref,
    lon_ref, lat_ref, stack_ref,
):
    height, width = alpha_ref.shape[1], alpha_ref.shape[2]
    ext = height + 2 * HB

    @pl.when(pl.program_id(0) == 0)
    def _():
        for level in range(2):
            spread = width_ref[level].astype(F32)
            source = iota((width, width), 0)
            high, low = split(taps(source - iota((width, width), 1), spread))
            lane = iota((LANES, width), 0)
            edge = taps(packed_column(lane, level, width) - iota((LANES, width), 1), spread)
            for t in range(MEMBERS):
                part_high, part_low = split(jnp.where(packed_member(lane) == t, edge, 0.0))
                lon_ref[level, t, :width, :width] = high
                lon_ref[level, t, :width, width:] = low
                lon_ref[level, t, width:, :width] = part_high
                lon_ref[level, t, width:, width:] = part_low
            source = row_of(iota((height, ext), 1), height)
            high, low = split(taps(source - iota((height, ext), 0), spread))
            lat_ref[level, :, :ext] = high
            lat_ref[level, :, ext : 2 * ext] = low
            lat_ref[level, :, 2 * ext :] = high

    half = iota((ext, LANES), 1) < LANES // 2

    def stacked(value):
        high, low = split(value)
        return jnp.concatenate([high, high, low], 0)

    for level in range(2):
        west = west_ref[0].astype(F32)
        east = east_ref[0].astype(F32)
        cell = jnp.where(half, west, east) if level == 0 else jnp.where(half, east, west)
        side = dot(lat_ref[level], stacked(cell * edge_ref[level]))
        side = jnp.concatenate(split(side), 0)
        for p in range(MEMBERS // 2):
            columns = []
            for t in (2 * p, 2 * p + 1):
                k = 2 * t + level
                field = jnp.concatenate(
                    [perts_ref[k].astype(F32), above_ref[k].astype(F32), below_ref[k].astype(F32)], 0
                )
                columns.append(stacked(field * own_ref[level]))
            both = dot(lat_ref[level], jnp.concatenate(columns, 1))
            for number in range(2):
                k = 2 * (2 * p + number) + level
                high, low = split(both[:, number * width : (number + 1) * width])
                stack_ref[k, :height, :width] = high
                stack_ref[k, height:, :width] = low
                stack_ref[k, :, width:] = side
    for level in range(2):
        for t in range(MEMBERS):
            k = 2 * t + level
            both = dot(stack_ref[k], lon_ref[level, t])
            total = both[:height, :width] + both[:height, width:] + both[height:, :width]
            out_ref[k] = alpha_ref[k].astype(F32) + total


def GRAD_SCRATCH(height, width):
    ext = height + 2 * HB
    return [
        pltpu.VMEM((2, MEMBERS, width + LANES, 2 * width), BF16),
        pltpu.VMEM((2, height, 3 * ext), BF16),
        pltpu.VMEM((GROUP, 2 * height, width + LANES), BF16),
    ]


def exchange(to_next, to_previous, axis):
    count = lax.axis_size(axis)
    forward = [(i, (i + 1) % count) for i in range(count)]
    backward = [(target, source) for source, target in forward]
    ahead = lax.ppermute(to_next, axis, forward)
    behind = lax.ppermute(to_previous, axis, backward)
    return ahead, behind


def vmem(*shape):
    return pl.BlockSpec(shape, lambda s: (0,) * len(shape))


def grouped(*shape):
    return pl.BlockSpec(shape, lambda s: (s,) + (0,) * (len(shape) - 1))


def shaped(shape, dtype=F32):
    return jax.ShapeDtypeStruct(shape, dtype)


def whole_step(
    alpha_fields,
    member_perts,
    band_widths,
    lat_index,
    lat_weight,
    lon_index,
    lon_weight,
    innovation,
    obs_weight,
):
    members, levels, height, width = alpha_fields.shape
    fields = members * levels
    groups = fields // GROUP
    ext = height + 2 * HB
    fine_h, fine_w = innovation.shape[1], innovation.shape[2]
    alpha = alpha_fields.reshape(fields, height, width)
    perts = member_perts.reshape(fields, height, width)
    smem = pl.BlockSpec(memory_space=pltpu.SMEM)
    anywhere = pl.BlockSpec(memory_space=pl.ANY)
    scale = width // LANES
    lanes = rounded(width + 2 * HB, LANES)
    tall = rounded(ext + 2 * STRIP, LANES)

    def call(kernel, out_shape, flops=10**8, grant=4, **more):
        semantics = ("arbitrary",) if "grid" in more else ()
        return pl.pallas_call(
            kernel,
            out_shape=out_shape,
            compiler_params=pltpu.CompilerParams(
                dimension_semantics=semantics, vmem_limit_bytes=min(60, grant * scale) * 1024 * 1024
            ),
            cost_estimate=pl.CostEstimate(flops=flops, bytes_accessed=10**6, transcendentals=0),
            **more,
        )

    edge = shaped((fields, HB, width), BF16)
    to_next, to_previous = call(
        rows_kernel,
        [edge, edge],
        in_specs=[pl.BlockSpec(memory_space=pltpu.HBM)],
        out_specs=[pl.BlockSpec(memory_space=pltpu.VMEM)] * 2,
        scratch_shapes=[pltpu.SemaphoreType.DMA((2,))],
    )(perts)
    above, below = exchange(to_next, to_previous, "gy")

    side = shaped((4 * SKIRT + 8, fine_h))
    to_next, to_previous = call(fine_cols_kernel, [side, side])(
        innovation, obs_weight, lon_index, lon_weight
    )
    fine_west, fine_east = exchange(to_next, to_previous, "gx")

    packed = shaped((groups, ext, LANES), BF16)
    to_next, to_previous = call(
        pack_kernel,
        [packed, packed],
        grant=8,
        grid=(groups,),
        in_specs=[grouped(GROUP, height, width)] + [grouped(GROUP, HB, width)] * 2,
        out_specs=[grouped(1, ext, LANES)] * 2,
    )(perts, above, below)
    west, east = exchange(to_next, to_previous, "gx")

    strip = shaped((8 * SKIRT + 8, fine_w))
    whole = pl.BlockSpec(memory_space=pltpu.VMEM)
    to_next, to_previous, token = call(
        fine_rows_kernel, [strip, strip, shaped((8, LANES))], in_specs=[whole] * 6 + [anywhere]
    )(innovation, obs_weight, lat_index, lat_weight, fine_west, fine_east, to_next)
    fine_above, fine_below = exchange(to_next, to_previous, "gy")

    partial, edge_rows, edge_cols = call(
        local_kernel,
        [
            shaped((2, height, width)),
            shaped((fields, 2 * HB, width)),
            shaped((groups, 2, ext, LANES)),
        ],
        flops=10**10,
        grant=16,
        grid=(groups,),
        in_specs=[
            smem,
            grouped(GROUP, height, width),
            grouped(GROUP, height, width),
            anywhere,
        ],
        out_specs=[
            vmem(2, height, width),
            grouped(GROUP, 2 * HB, width),
            grouped(1, 2, ext, LANES),
        ],
        scratch_shapes=[
            pltpu.VMEM((2, MEMBERS, 2 * width, width + LANES), BF16),
            pltpu.VMEM((2, ext, 3 * height), BF16),
            pltpu.VMEM((2, 3 * height, MEMBERS * width + LANES), BF16),
        ],
    )(band_widths, alpha, perts, token)

    framed = call(
        frame_kernel, shaped((2, ext, width + LANES)), in_specs=[whole] * 7
    )(partial, edge_rows, edge_cols, above, below, west, east)
    count = lax.axis_size("ma")
    other = lax.ppermute(framed, "ma", [(i, (i + 1) % count) for i in range(count)])
    strip = shaped((2, STRIP, lanes))
    framed, to_next, to_previous = call(
        total_kernel, [shaped((2, ext, lanes)), strip, strip]
    )(framed, other)
    north, south = exchange(to_next, to_previous, "gy")
    strip = shaped((2 * STRIP, tall))
    stack, to_next, to_previous = call(
        functools.partial(strips_kernel, width), [shaped((2, tall, lanes)), strip, strip]
    )(framed, north, south)
    strip_west, strip_east = exchange(to_next, to_previous, "gx")

    lon_total = width * lax.axis_size("gx")
    everything = [pl.BlockSpec(memory_space=pltpu.VMEM)] * 13
    increment, own, edge = call(
        functools.partial(fine_kernel, lon_total),
        [shaped((2, fine_h, fine_w)), shaped((2, ext, width)), shaped((2, ext, LANES))],
        grant=16,
        in_specs=everything,
        scratch_shapes=[
            pltpu.VMEM((fine_h + LANES, lanes + LANES), F32),
            pltpu.VMEM((fine_h + LANES, fine_w), F32),
        ],
    )(
        stack,
        strip_west,
        strip_east,
        innovation,
        obs_weight,
        lat_index,
        lat_weight,
        lon_index,
        lon_weight,
        fine_west,
        fine_east,
        fine_above,
        fine_below,
    )

    gradient = call(
        gradient_kernel,
        shaped((fields, height, width)),
        grant=16,
        grid=(groups,),
        in_specs=[
            smem,
            grouped(GROUP, height, width),
            grouped(GROUP, height, width),
            grouped(GROUP, HB, width),
            grouped(GROUP, HB, width),
            grouped(1, ext, LANES),
            grouped(1, ext, LANES),
            vmem(2, ext, width),
            vmem(2, ext, LANES),
        ],
        out_specs=grouped(GROUP, height, width),
        scratch_shapes=GRAD_SCRATCH(height, width),
    )(band_widths, alpha, perts, above, below, west, east, own, edge)
    return increment, gradient.reshape(alpha_fields.shape)


def solution(mesh):
    placed = (
        P("ma", None, "gy", "gx"),
        P("ma", None, "gy", "gx"),
        P(),
        P("gy"),
        P("gy"),
        P("gx"),
        P("gx"),
        P(None, "gy", "gx"),
        P(None, "gy", "gx"),
    )
    return jax.shard_map(
        whole_step,
        mesh=mesh,
        in_specs=placed,
        out_specs=(P(None, "gy", "gx"), P("ma", None, "gy", "gx")),
        check_vma=False,
    )
```

```python
import functools

import jax
import jax.numpy as jnp
from jax import lax
from jax.experimental import pallas as pl
from jax.experimental.pallas import tpu as pltpu
from jax.sharding import PartitionSpec as P

HB = 8
GROUP = 16
MEMBERS = 8
SKIRT = 24
STRIP = 24
NOWHERE = -9999
LANES = 128
F32 = jnp.float32
BF16 = jnp.bfloat16


def rounded(size, step):
    return -(-size // step) * step


def iota(shape, axis):
    return lax.broadcasted_iota(jnp.int32, shape, axis)


def split(value):
    high = value.astype(BF16)
    return high, (value - high.astype(F32)).astype(BF16)


def dot(left, right, dims=(1, 0)):
    return lax.dot_general(
        left, right, (((dims[0],), (dims[1],)), ((), ())), preferred_element_type=F32
    )


def dot3(left, right, dims=(1, 0)):
    left_high, left_low = left if isinstance(left, tuple) else split(left)
    right_high, right_low = right if isinstance(right, tuple) else split(right)
    total = dot(left_high, right_low, dims) + dot(left_low, right_high, dims)
    return total + dot(left_high, right_high, dims)


def row_of(index, height):
    above = index - height - HB
    return jnp.where(index < height, index, jnp.where(index < height + HB, above, index - HB))


def packed_column(lane, level, width):
    west = (lane < LANES // 2) if level == 0 else (lane >= LANES // 2)
    cell = lane & (HB - 1)
    return jnp.where(west, cell - HB, width + cell)


def packed_member(lane):
    return (lane & (LANES // 2 - 1)) >> 3


def taps(offset, spread):
    lane = iota((8, LANES), 1)
    distance = (lane - HB).astype(F32)
    scale = jnp.full((8, LANES), 1.0, F32) * (0.5 / (spread * spread))
    shape = jnp.where(lane <= 2 * HB, jnp.exp(-(distance * distance) * scale), 0.0)
    norm = lax.rsqrt(jnp.sum(shape * shape, axis=1, keepdims=True))[:1, :1]
    far = offset.astype(F32)
    value = jnp.exp(-(far * far) * scale[:1, :1]) * norm
    return jnp.where(jnp.abs(offset) <= HB, value, 0.0)


def tables_kernel(turned, width_ref, lon_ref, lat_ref):
    if turned:
        height, ext = lat_ref.shape[1], lat_ref.shape[2] // 3
        width = lon_ref.shape[3] // 2
    else:
        ext, height = lat_ref.shape[1], lat_ref.shape[2] // 3
        width = lon_ref.shape[3] - LANES
    for level in range(2):
        spread = width_ref[level].astype(F32)
        high, low = split(taps(iota((width, width), 0) - iota((width, width), 1), spread))
        shape = (LANES, width) if turned else (width, LANES)
        lane = iota(shape, 1 - turned)
        edge = taps(iota(shape, int(turned)) - packed_column(lane, level, width), spread)
        for t in range(MEMBERS):
            part_high, part_low = split(jnp.where(packed_member(lane) == t, edge, 0.0))
            lon_ref[level, t, :width, :width] = high
            lon_ref[level, t, width:, width:] = part_low
            if turned:
                lon_ref[level, t, :width, width:] = low
                lon_ref[level, t, width:, :width] = part_high
            else:
                lon_ref[level, t, width:, :width] = low
                lon_ref[level, t, :width, width:] = part_high
        shape = (height, ext) if turned else (ext, height)
        framed = row_of(iota(shape, int(turned)), height)
        high, low = split(taps(framed - iota(shape, 1 - turned), spread))
        size = shape[1]
        lat_ref[level, :, :size] = high
        lat_ref[level, :, size : 2 * size] = low
        lat_ref[level, :, 2 * size :] = high


def pack_kernel(perts_ref, even_ref, odd_ref, east_ref, west_ref, above_ref, below_ref):
    rows = east_ref.shape[1]
    turned = lax.axis_index("gy") % 2 == 1
    width = perts_ref.shape[2]
    lane = iota((rows, LANES), 1)
    east = jnp.zeros((rows, LANES), F32)
    west = jnp.zeros((rows, LANES), F32)
    for k in range(GROUP):
        t, level = k // 2, k % 2
        own = perts_ref[k]
        even, odd = even_ref[k].astype(F32), odd_ref[k].astype(F32)
        above = jnp.where(turned, even, odd)
        below = jnp.where(turned, odd, even)
        above_ref[k] = above.astype(BF16)
        below_ref[k] = below.astype(BF16)
        whole = jnp.concatenate([own.astype(F32), above, below], 0)
        last = whole[:, width - LANES :]
        first = whole[:, :LANES]
        slot = level * (LANES // 2) + t * HB
        other = (1 - level) * (LANES // 2) + t * HB
        last = pltpu.roll(last, (slot + HB) % LANES, 1)
        first = first if other == 0 else pltpu.roll(first, other, 1)
        east = jnp.where(lane >> 3 == slot // HB, last, east)
        west = jnp.where(lane >> 3 == other // HB, first, west)
    east_ref[0] = east.astype(BF16)
    west_ref[0] = west.astype(BF16)


def local_kernel(
    alpha_ref, perts_ref, lon_ref, lat_ref, token_ref, sum_ref, rows_ref, cols_ref, stack_ref
):
    height, width = alpha_ref.shape[1], alpha_ref.shape[2]

    @pl.when(pl.program_id(0) == 0)
    def _():
        sum_ref[...] = jnp.zeros_like(sum_ref)

    def put(level, start, value):
        high, low = split(value)
        stop = start + value.shape[1]
        stack_ref[level, :height, start:stop] = high
        stack_ref[level, height : 2 * height, start:stop] = high
        stack_ref[level, 2 * height :, start:stop] = low

    for level in range(2):
        packed = jnp.zeros((height, LANES), F32)
        for t in range(MEMBERS):
            field = alpha_ref[2 * t + level]
            both = dot(jnp.concatenate([field, field], 1), lon_ref[level, t])
            put(level, t * width, both[:, :width])
            packed = packed + both[:, width:]
        put(level, MEMBERS * width, packed)
    for level in range(2):
        total = sum_ref[level]
        for pair in range(MEMBERS // 2):
            base = 2 * pair * width
            wide = dot(lat_ref[level], stack_ref[level, :, base : base + 2 * width])
            for side in range(2):
                k = 2 * (2 * pair + side) + level
                field = wide[:, side * width : (side + 1) * width]
                total = total + perts_ref[k].astype(F32) * field[:height]
                rows_ref[k] = field[height:]
        sum_ref[level] = total
        cols_ref[0, level] = dot(lat_ref[level], stack_ref[level, :, MEMBERS * width :])


def stacked_cell(index, size, base):
    cell = row_of(index, size)
    low = index - base
    cell = jnp.where(index < size + 2 * HB, cell, NOWHERE)
    cell = jnp.where((low >= 0) & (low < STRIP), low - 2 * HB, cell)
    return jnp.where((low >= STRIP) & (low < 2 * STRIP), low - STRIP + size - HB, cell)


def interpolate(cell, index, weight):
    near = jnp.where(cell == index, 1.0 - weight, 0.0)
    return near + jnp.where(cell == index + 1, weight, 0.0)


def seal(axis, next_ref, previous_ref):
    place = lax.axis_index(axis)

    @pl.when(place == lax.axis_size(axis) - 1)
    def _():
        next_ref[...] = jnp.zeros_like(next_ref)

    @pl.when(place == 0)
    def _():
        previous_ref[...] = jnp.zeros_like(previous_ref)


def rows_kernel(perts_ref, even_ref, odd_ref, sems):
    height = perts_ref.shape[1]
    place = lax.axis_index("gy")

    def fill(even, odd):
        copies = [
            pltpu.make_async_copy(perts_ref.at[:, even : even + HB], even_ref, sems.at[0]),
            pltpu.make_async_copy(perts_ref.at[:, odd : odd + HB], odd_ref, sems.at[1]),
        ]
        for copy in copies:
            copy.start()
        for copy in copies:
            copy.wait()

    @pl.when(place % 2 == 0)
    def _():
        fill(height - HB, 0)

    @pl.when(place % 2 == 1)
    def _():
        fill(0, height - HB)

    @pl.when((place == 0) | (place == lax.axis_size("gy") - 1))
    def _():
        odd_ref[...] = jnp.zeros_like(odd_ref)


def table(index, weight):
    size = index.shape[-1]
    row = iota((8, size), 0)
    return jnp.where(
        row == 0, index.astype(F32).reshape(1, size), jnp.where(row == 1, weight.reshape(1, size), 0.0)
    )


def fine_cols_kernel(target_ref, weight_ref, index_ref, share_ref, east_ref, west_ref):
    cols = target_ref.shape[2]
    for a, ref in enumerate((target_ref, weight_ref)):
        for level in range(2):
            start = (2 * a + level) * SKIRT
            east_ref[start : start + SKIRT] = ref[level, :, cols - LANES :].T[LANES - SKIRT :]
            west_ref[start : start + SKIRT] = ref[level, :, :LANES].T[:SKIRT]
    lon = table(index_ref[...], share_ref[...])
    east_ref[4 * SKIRT :, :LANES] = lon[:, cols - LANES :]
    west_ref[4 * SKIRT :, :LANES] = lon[:, :LANES]


def fine_rows_kernel(
    target_ref, weight_ref, index_ref, share_ref, west_ref, east_ref, order_ref, next_ref, previous_ref,
    token_ref,
):
    rows = target_ref.shape[1]
    for a, ref in enumerate((target_ref, weight_ref)):
        for level in range(2):
            start = (2 * a + level) * SKIRT
            next_ref[start : start + SKIRT] = ref[level, rows - SKIRT :]
            previous_ref[start : start + SKIRT] = ref[level, :SKIRT]
    lat = table(index_ref[...], share_ref[...])
    for side, ref in enumerate((west_ref, east_ref)):
        lanes = slice(side * LANES, (side + 1) * LANES)
        next_ref[4 * SKIRT : 8 * SKIRT, lanes] = ref[: 4 * SKIRT, rows - LANES :]
        previous_ref[4 * SKIRT : 8 * SKIRT, lanes] = ref[: 4 * SKIRT, :LANES]
    next_ref[8 * SKIRT :, :LANES] = lat[:, rows - LANES :]
    previous_ref[8 * SKIRT :, :LANES] = lat[:, :LANES]
    token_ref[...] = lat[:, :LANES]
    seal("gy", next_ref, previous_ref)


def frame_kernel(
    sum_ref, rows_ref, cols_ref, above_ref, below_ref, west_ref, east_ref, out_ref
):
    height, width = sum_ref.shape[1], sum_ref.shape[2]
    ext = height + 2 * HB
    groups = west_ref.shape[0]
    half = iota((ext, LANES), 1) < LANES // 2
    for level in range(2):
        edge = jnp.zeros((2 * HB, width), F32)
        packed = jnp.zeros((ext, LANES), F32)
        for group in range(groups):
            for t in range(MEMBERS):
                k = group * GROUP + 2 * t + level
                halo = jnp.concatenate([above_ref[k].astype(F32), below_ref[k].astype(F32)], 0)
                edge = edge + halo * rows_ref[k]
            west = west_ref[group].astype(F32)
            east = east_ref[group].astype(F32)
            cell = jnp.where(half, west, east) if level == 0 else jnp.where(half, east, west)
            packed = packed + cell * cols_ref[group, level]
        column = packed_column(iota((LANES, LANES), 0), level, width)
        slot = iota((LANES, LANES), 1)
        target = jnp.where(slot < HB, slot - HB, jnp.where(slot < 2 * HB, slot - HB + width, NOWHERE))
        gather = (column == target).astype(BF16)
        high, low = split(packed)
        out_ref[level, :height, :width] = sum_ref[level]
        out_ref[level, height:, :width] = edge
        out_ref[level, :, width:] = dot(high, gather) + dot(low, gather)


def total_kernel(mine_ref, other_ref, total_ref, next_ref, previous_ref):
    total = mine_ref[...] + other_ref[...]
    height = total.shape[1] - 2 * HB
    total_ref[...] = total
    next_ref[:, : 2 * HB] = total[:, height - 2 * HB : height]
    next_ref[:, 2 * HB :] = total[:, height + HB :]
    previous_ref[:, :HB] = total[:, height : height + HB]
    previous_ref[:, HB:] = total[:, : 2 * HB]
    seal("gy", next_ref, previous_ref)


def strips_kernel(width, total_ref, above_ref, below_ref, stack_ref, east_ref, west_ref):
    ext, lanes = total_ref.shape[1], total_ref.shape[2]
    rows = stack_ref.shape[1]
    column = stacked_cell(iota((STRIP, lanes), 1), width, lanes)
    number = iota((STRIP, lanes), 0)
    pick_east = (column == number + width - 2 * HB).astype(BF16)
    pick_west = (column == number - HB).astype(BF16)
    for level in range(2):
        stack_ref[level, :ext] = total_ref[level]
        stack_ref[level, ext : ext + STRIP] = above_ref[level]
        stack_ref[level, ext + STRIP : ext + 2 * STRIP] = below_ref[level]
        stack_ref[level, ext + 2 * STRIP :] = jnp.zeros((rows - ext - 2 * STRIP, lanes), F32)
        high, low = split(stack_ref[level])
        part = slice(level * STRIP, (level + 1) * STRIP)
        east_ref[part] = dot(pick_east, high, (1, 1)) + dot(pick_east, low, (1, 1))
        west_ref[part] = dot(pick_west, high, (1, 1)) + dot(pick_west, low, (1, 1))


def fine_maps_kernel(
    height,
    width,
    lon_total,
    stack_ref,
    lat_index_ref,
    lat_share_ref,
    lon_index_ref,
    lon_share_ref,
    west_ref,
    east_ref,
    above_ref,
    below_ref,
    part_ref,
    beyond_ref,
    lat_map_ref,
    strip_map_ref,
    side_map_ref,
    lat_back_ref,
    back_ref,
    side_back_ref,
    side_target_ref,
    side_weight_ref,
):
    ext = height + 2 * HB
    span, cols = part_ref.shape[1], part_ref.shape[2]
    tall, lanes = stack_ref.shape[1], stack_ref.shape[2]
    lane = iota((8, LANES), 1)
    first = iota((8, LANES), 0) == 0

    def side(low, high):
        low = pltpu.roll(low, SKIRT, 1)
        high = pltpu.roll(high, SKIRT, 1)
        blank = jnp.where(first, 1.0e6, 0.0)
        return jnp.where(lane < SKIRT, low, jnp.where(lane < 2 * SKIRT, high, blank))

    def corner(low, high):
        spot = iota(low.shape, 1)
        low = pltpu.roll(low, SKIRT, 1)
        high = pltpu.roll(high, SKIRT, 1)
        return jnp.where(spot < SKIRT, low, jnp.where(spot < 2 * SKIRT, high, 0.0))

    def keep(ref, value):
        high, low = split(value)
        ref[0] = high
        ref[1] = low
        return high, low

    lat_side = side(above_ref[8 * SKIRT :, :LANES], below_ref[8 * SKIRT :, :LANES])
    lat = jnp.concatenate([table(lat_index_ref[...], lat_share_ref[...]), lat_side], 1)
    lon_side = side(west_ref[4 * SKIRT :, :LANES], east_ref[4 * SKIRT :, :LANES])
    lon = jnp.concatenate([table(lon_index_ref[...], lon_share_ref[...]), lon_side], 1)
    lat_cell = lat[0:1].astype(jnp.int32) - lax.axis_index("gy") * height
    lat_share = lat[1:2]
    lon_cell = lon[0:1].astype(jnp.int32) - lax.axis_index("gx") * width
    lon_cell = jnp.where(lon_cell < -(lon_total // 2), lon_cell + lon_total, lon_cell)
    wrap = (lon_cell >= lon_total // 2) & (lon_cell < lon_total)
    lon_cell = jnp.where(wrap, lon_cell - lon_total, lon_cell)
    lon_share = lon[1:2]
    upright = jnp.concatenate([lat_cell.astype(F32), lat_share, jnp.zeros((6, span), F32)], 0).T
    lat_cell_up, lat_share_up = upright[:, 0:1].astype(jnp.int32), upright[:, 1:2]
    upright = jnp.concatenate(
        [lon_cell.astype(F32), lon_share, jnp.zeros((6, cols + LANES), F32)], 0
    ).T
    lon_cell_up, lon_share_up = upright[:, 0:1].astype(jnp.int32), upright[:, 1:2]
    beside = slice(cols, cols + 2 * SKIRT)

    lat_map = keep(
        lat_map_ref,
        interpolate(stacked_cell(iota((span, tall), 1), height, ext), lat_cell_up, lat_share_up),
    )
    broad = lanes + LANES
    lon_map = interpolate(
        stacked_cell(iota((broad, cols), 0), width, lanes), lon_cell[:, :cols], lon_share[:, :cols]
    )
    keep(strip_map_ref, lon_map[lanes:])
    lon_map = split(lon_map[:lanes])
    side_map = interpolate(
        stacked_cell(iota((2 * SKIRT, broad), 1), width, lanes),
        lon_cell_up[beside],
        lon_share_up[beside],
    )
    keep(side_map_ref, side_map[:, lanes:])
    side_map = split(side_map[:, :lanes])
    keep(lat_back_ref, interpolate(row_of(iota((ext, span), 0), height), lat_cell, lat_share))
    for level in range(2):
        wide = split(dot3(lat_map, stack_ref[level]))
        part_ref[level] = dot3(wide, lon_map)
        beyond_ref[level] = dot3(side_map, wide, (1, 1))
        lane_wide = iota((1, width + LANES), 1)
        column = jnp.where(
            lane_wide < width, lane_wide, packed_column(lane_wide - width, level, width)
        )
        keep(back_ref.at[level], interpolate(column, lon_cell_up[:cols], lon_share_up[:cols]))
        keep(side_back_ref.at[level], interpolate(column, lon_cell_up[beside], lon_share_up[beside]))
        for array, out_ref in enumerate((side_target_ref, side_weight_ref)):
            start = (2 * array + level) * SKIRT
            for number, ref in enumerate((west_ref, east_ref)):
                tile = slice(number * LANES, (number + 1) * LANES)
                rows = slice(4 * SKIRT + start, 5 * SKIRT + start)
                at = slice(number * SKIRT, (number + 1) * SKIRT)
                out_ref[level, at, : span - LANES] = ref[start : start + SKIRT]
                out_ref[level, at, span - LANES :] = corner(above_ref[rows, tile], below_ref[rows, tile])


def fine_kernel(
    strip_west_ref,
    strip_east_ref,
    target_ref,
    weight_ref,
    above_ref,
    below_ref,
    part_ref,
    beyond_ref,
    lat_map_ref,
    strip_map_ref,
    side_map_ref,
    lat_back_ref,
    back_ref,
    side_back_ref,
    side_target_ref,
    side_weight_ref,
    inc_ref,
    own_ref,
    edge_ref,
    wide_ref,
    miss_ref,
):
    width = own_ref.shape[2]
    rows, cols = target_ref.shape[1], target_ref.shape[2]
    span = part_ref.shape[1]
    wide_ref[...] = jnp.zeros_like(wide_ref)
    blank = jnp.zeros((span - rows - 2 * SKIRT, cols), F32)
    miss_ref[0, rows + 2 * SKIRT :] = blank
    miss_ref[1, rows + 2 * SKIRT :] = blank

    def kept(ref):
        return ref[0], ref[1]

    for level in range(2):
        part = slice(level * STRIP, (level + 1) * STRIP)
        strips = jnp.concatenate([strip_west_ref[part], strip_east_ref[part]], 0)
        wide_ref[level, :, : 2 * STRIP] = dot3(kept(lat_map_ref), strips, (1, 1))
        wide = split(wide_ref[level])
        increment = part_ref[level] + dot3(wide, kept(strip_map_ref))
        inc_ref[level] = increment[:rows]
        miss_ref[level, :rows] = weight_ref[level] * (increment[:rows] - target_ref[level])
        target_rows = slice(level * SKIRT, (level + 1) * SKIRT)
        weight_rows = slice((2 + level) * SKIRT, (3 + level) * SKIRT)
        for number, ref in enumerate((above_ref, below_ref)):
            start = rows + number * SKIRT
            difference = increment[start : start + SKIRT] - ref[target_rows]
            miss_ref[level, start : start + SKIRT] = ref[weight_rows] * difference
        beyond = beyond_ref[level] + dot3(kept(side_map_ref), wide, (1, 1))
        beyond = side_weight_ref[level] * (beyond - side_target_ref[level])
        by_lon = dot3(miss_ref[level], kept(back_ref.at[level]))
        by_lon = by_lon + dot3(beyond, kept(side_back_ref.at[level]), (0, 0))
        residual = dot3(kept(lat_back_ref), by_lon)
        own_ref[level] = residual[:, :width]
        edge_ref[level] = residual[:, width:]


def gradient_kernel(
    alpha_ref, perts_ref, above_ref, below_ref, west_ref, east_ref, own_ref, edge_ref, lon_ref, lat_ref,
    out_ref, stack_ref,
):
    height, width = alpha_ref.shape[1], alpha_ref.shape[2]
    ext = height + 2 * HB

    half = iota((ext, LANES), 1) < LANES // 2

    def stacked(value):
        high, low = split(value)
        return jnp.concatenate([high, high, low], 0)

    for level in range(2):
        west = west_ref[0].astype(F32)
        east = east_ref[0].astype(F32)
        cell = jnp.where(half, west, east) if level == 0 else jnp.where(half, east, west)
        side = dot(lat_ref[level], stacked(cell * edge_ref[level]))
        side = jnp.concatenate(split(side), 0)
        for p in range(MEMBERS // 2):
            columns = []
            for t in (2 * p, 2 * p + 1):
                k = 2 * t + level
                field = jnp.concatenate(
                    [perts_ref[k].astype(F32), above_ref[k].astype(F32), below_ref[k].astype(F32)], 0
                )
                columns.append(stacked(field * own_ref[level]))
            both = dot(lat_ref[level], jnp.concatenate(columns, 1))
            for number in range(2):
                k = 2 * (2 * p + number) + level
                high, low = split(both[:, number * width : (number + 1) * width])
                stack_ref[k, :height, :width] = high
                stack_ref[k, height:, :width] = low
                stack_ref[k, :, width:] = side
    for level in range(2):
        for t in range(MEMBERS):
            k = 2 * t + level
            both = dot(stack_ref[k], lon_ref[level, t])
            total = both[:height, :width] + both[:height, width:] + both[height:, :width]
            out_ref[k] = alpha_ref[k].astype(F32) + total


def exchange(to_next, to_previous, axis):
    count = lax.axis_size(axis)
    forward = [(i, (i + 1) % count) for i in range(count)]
    backward = [(target, source) for source, target in forward]
    ahead = lax.ppermute(to_next, axis, forward)
    behind = lax.ppermute(to_previous, axis, backward)
    return ahead, behind


def exchange_pairs(to_even, to_odd, axis):
    count = lax.axis_size(axis)
    even = [(i, i ^ 1) for i in range(count)]
    odd = [(i, min(max(i + 1 if i % 2 else i - 1, 0), count - 1)) for i in range(count)]
    ahead = lax.ppermute(to_even, axis, even)
    behind = lax.ppermute(to_odd, axis, odd)
    return ahead, behind


def vmem(*shape):
    return pl.BlockSpec(shape, lambda s: (0,) * len(shape))


def grouped(*shape):
    return pl.BlockSpec(shape, lambda s: (s,) + (0,) * (len(shape) - 1))


def shaped(shape, dtype=F32):
    return jax.ShapeDtypeStruct(shape, dtype)


def whole_step(
    alpha_fields,
    member_perts,
    band_widths,
    lat_index,
    lat_weight,
    lon_index,
    lon_weight,
    innovation,
    obs_weight,
):
    members, levels, height, width = alpha_fields.shape
    fields = members * levels
    groups = fields // GROUP
    ext = height + 2 * HB
    fine_h, fine_w = innovation.shape[1], innovation.shape[2]
    alpha = alpha_fields.reshape(fields, height, width)
    perts = member_perts.reshape(fields, height, width)
    smem = pl.BlockSpec(memory_space=pltpu.SMEM)
    anywhere = pl.BlockSpec(memory_space=pl.ANY)
    whole = pl.BlockSpec(memory_space=pltpu.VMEM)
    scale = width // LANES
    lanes = rounded(width + 2 * HB, LANES)
    tall = rounded(ext + 2 * STRIP, LANES)

    def call(kernel, out_shape, flops=10**8, grant=4, **more):
        semantics = ("arbitrary",) if "grid" in more else ()
        return pl.pallas_call(
            kernel,
            out_shape=out_shape,
            compiler_params=pltpu.CompilerParams(
                dimension_semantics=semantics, vmem_limit_bytes=min(60, grant * scale) * 1024 * 1024
            ),
            cost_estimate=pl.CostEstimate(flops=flops, bytes_accessed=10**6, transcendentals=0),
            **more,
        )

    edge = shaped((fields, HB, width), BF16)
    to_even, to_odd = call(
        rows_kernel,
        [edge, edge],
        in_specs=[pl.BlockSpec(memory_space=pltpu.HBM)],
        out_specs=[pl.BlockSpec(memory_space=pltpu.VMEM)] * 2,
        scratch_shapes=[pltpu.SemaphoreType.DMA((2,))],
    )(perts)
    even, odd = exchange_pairs(to_even, to_odd, "gy")
    lon_shape, lat_shape = (2, MEMBERS, 2 * width, width + LANES), (2, ext, 3 * height)
    lon_back_shape, lat_back_shape = (2, MEMBERS, width + LANES, 2 * width), (2, height, 3 * ext)
    lon_table, lat_table = call(
        functools.partial(tables_kernel, False),
        [shaped(lon_shape, BF16), shaped(lat_shape, BF16)],
        grant=8,
        in_specs=[smem],
    )(band_widths)

    side = shaped((4 * SKIRT + 8, fine_h))
    to_next, to_previous = call(fine_cols_kernel, [side, side])(
        innovation, obs_weight, lon_index, lon_weight
    )
    fine_west, fine_east = exchange(to_next, to_previous, "gx")

    packed = shaped((groups, ext, LANES), BF16)
    to_next, to_previous, above, below = call(
        pack_kernel,
        [packed, packed, edge, edge],
        grant=8,
        grid=(groups,),
        in_specs=[grouped(GROUP, height, width)] + [grouped(GROUP, HB, width)] * 2,
        out_specs=[grouped(1, ext, LANES)] * 2 + [grouped(GROUP, HB, width)] * 2,
    )(perts, even, odd)
    west, east = exchange(to_next, to_previous, "gx")

    strip = shaped((8 * SKIRT + 8, fine_w))
    to_next, to_previous, token = call(
        fine_rows_kernel, [strip, strip, shaped((8, LANES))], in_specs=[whole] * 6 + [anywhere]
    )(innovation, obs_weight, lat_index, lat_weight, fine_west, fine_east, to_next)
    fine_above, fine_below = exchange(to_next, to_previous, "gy")

    partial, edge_rows, edge_cols = call(
        local_kernel,
        [
            shaped((2, height, width)),
            shaped((fields, 2 * HB, width)),
            shaped((groups, 2, ext, LANES)),
        ],
        flops=10**10,
        grant=16,
        grid=(groups,),
        in_specs=[
            grouped(GROUP, height, width),
            grouped(GROUP, height, width),
            whole,
            whole,
            anywhere,
        ],
        out_specs=[
            vmem(2, height, width),
            grouped(GROUP, 2 * HB, width),
            grouped(1, 2, ext, LANES),
        ],
        scratch_shapes=[
            pltpu.VMEM((2, 3 * height, MEMBERS * width + LANES), BF16),
        ],
    )(alpha, perts, lon_table, lat_table, token)

    framed = call(
        frame_kernel, shaped((2, ext, width + LANES)), in_specs=[whole] * 7
    )(partial, edge_rows, edge_cols, above, below, west, east)
    count = lax.axis_size("ma")
    other = lax.ppermute(framed, "ma", [(i, (i + 1) % count) for i in range(count)])
    strip = shaped((2, STRIP, lanes))
    framed, to_next, to_previous = call(
        total_kernel, [shaped((2, ext, lanes)), strip, strip]
    )(framed, other)
    lon_back, lat_back = call(
        functools.partial(tables_kernel, True),
        [shaped(lon_back_shape, BF16), shaped(lat_back_shape, BF16)],
        grant=8,
        in_specs=[smem],
    )(band_widths)
    north, south = exchange(to_next, to_previous, "gy")
    strip = shaped((2 * STRIP, tall))
    stack, to_next, to_previous = call(
        functools.partial(strips_kernel, width), [shaped((2, tall, lanes)), strip, strip]
    )(framed, north, south)
    strip_west, strip_east = exchange(to_next, to_previous, "gx")

    lon_total = width * lax.axis_size("gx")
    span = fine_h + LANES
    pair = (2, 2 * SKIRT, span)
    maps = call(
        functools.partial(fine_maps_kernel, height, width, lon_total),
        [
            shaped((2, span, fine_w)),
            shaped(pair),
            shaped((2, span, tall), BF16),
            shaped((2, LANES, fine_w), BF16),
            shaped((2, 2 * SKIRT, LANES), BF16),
            shaped((2, ext, span), BF16),
            shaped((2, 2, fine_w, width + LANES), BF16),
            shaped((2, 2, 2 * SKIRT, width + LANES), BF16),
            shaped(pair),
            shaped(pair),
        ],
        grant=16,
        in_specs=[whole] * 9,
    )(
        stack,
        lat_index,
        lat_weight,
        lon_index,
        lon_weight,
        fine_west,
        fine_east,
        fine_above,
        fine_below,
    )
    increment, own, edge = call(
        fine_kernel,
        [shaped((2, fine_h, fine_w)), shaped((2, ext, width)), shaped((2, ext, LANES))],
        grant=16,
        in_specs=[whole] * 16,
        scratch_shapes=[pltpu.VMEM((2, span, LANES), F32), pltpu.VMEM((2, span, fine_w), F32)],
    )(strip_west, strip_east, innovation, obs_weight, fine_above, fine_below, *maps)

    gradient = call(
        gradient_kernel,
        shaped((fields, height, width)),
        grant=16,
        grid=(groups,),
        in_specs=[
            grouped(GROUP, height, width),
            grouped(GROUP, height, width),
            grouped(GROUP, HB, width),
            grouped(GROUP, HB, width),
            grouped(1, ext, LANES),
            grouped(1, ext, LANES),
            vmem(2, ext, width),
            vmem(2, ext, LANES),
            whole,
            whole,
        ],
        out_specs=grouped(GROUP, height, width),
        scratch_shapes=[pltpu.VMEM((GROUP, 2 * height, width + LANES), BF16)],
    )(alpha, perts, above, below, west, east, own, edge, lon_back, lat_back)
    return increment, gradient.reshape(alpha_fields.shape)


def solution(mesh):
    placed = (
        P("ma", None, "gy", "gx"),
        P("ma", None, "gy", "gx"),
        P(),
        P("gy"),
        P("gy"),
        P("gx"),
        P("gx"),
        P(None, "gy", "gx"),
        P(None, "gy", "gx"),
    )
    return jax.shard_map(
        whole_step,
        mesh=mesh,
        in_specs=placed,
        out_specs=(P(None, "gy", "gx"), P("ma", None, "gy", "gx")),
        check_vma=False,
    )
```

```python
import functools

import jax
import jax.numpy as jnp
from jax import lax
from jax.experimental import pallas as pl
from jax.experimental.pallas import tpu as pltpu
from jax.sharding import PartitionSpec as P

HB = 8
GROUP = 16
MEMBERS = 8
SKIRT = 24
STRIP = 24
NOWHERE = -9999
LANES = 128
F32 = jnp.float32
BF16 = jnp.bfloat16


def rounded(size, step):
    return -(-size // step) * step


def iota(shape, axis):
    return lax.broadcasted_iota(jnp.int32, shape, axis)


def split(value):
    high = value.astype(BF16)
    return high, (value - high.astype(F32)).astype(BF16)


def dot(left, right, dims=(1, 0)):
    return lax.dot_general(
        left, right, (((dims[0],), (dims[1],)), ((), ())), preferred_element_type=F32
    )


def dot3(left, right, dims=(1, 0)):
    left_high, left_low = left if isinstance(left, tuple) else split(left)
    right_high, right_low = right if isinstance(right, tuple) else split(right)
    total = dot(left_high, right_low, dims) + dot(left_low, right_high, dims)
    return total + dot(left_high, right_high, dims)


def row_of(index, height):
    above = index - height - HB
    return jnp.where(index < height, index, jnp.where(index < height + HB, above, index - HB))


def packed_column(lane, level, width):
    west = (lane < LANES // 2) if level == 0 else (lane >= LANES // 2)
    cell = lane & (HB - 1)
    return jnp.where(west, cell - HB, width + cell)


def packed_member(lane):
    return (lane & (LANES // 2 - 1)) >> 3


def taps(offset, spread):
    lane = iota((8, LANES), 1)
    distance = (lane - HB).astype(F32)
    scale = jnp.full((8, LANES), 1.0, F32) * (0.5 / (spread * spread))
    shape = jnp.where(lane <= 2 * HB, jnp.exp(-(distance * distance) * scale), 0.0)
    norm = lax.rsqrt(jnp.sum(shape * shape, axis=1, keepdims=True))[:1, :1]
    far = offset.astype(F32)
    value = jnp.exp(-(far * far) * scale[:1, :1]) * norm
    return jnp.where(jnp.abs(offset) <= HB, value, 0.0)


def tables_kernel(turned, width_ref, lon_ref, lat_ref):
    if turned:
        height, ext = lat_ref.shape[1], lat_ref.shape[2] // 3
        width = lon_ref.shape[3] // 2
    else:
        ext, height = lat_ref.shape[1], lat_ref.shape[2] // 3
        width = lon_ref.shape[3] - LANES
    for level in range(2):
        spread = width_ref[level].astype(F32)
        high, low = split(taps(iota((width, width), 0) - iota((width, width), 1), spread))
        shape = (LANES, width) if turned else (width, LANES)
        lane = iota(shape, 1 - turned)
        edge = taps(iota(shape, int(turned)) - packed_column(lane, level, width), spread)
        for t in range(MEMBERS):
            part_high, part_low = split(jnp.where(packed_member(lane) == t, edge, 0.0))
            lon_ref[level, t, :width, :width] = high
            lon_ref[level, t, width:, width:] = part_low
            if turned:
                lon_ref[level, t, :width, width:] = low
                lon_ref[level, t, width:, :width] = part_high
            else:
                lon_ref[level, t, width:, :width] = low
                lon_ref[level, t, :width, width:] = part_high
        shape = (height, ext) if turned else (ext, height)
        framed = row_of(iota(shape, int(turned)), height)
        high, low = split(taps(framed - iota(shape, 1 - turned), spread))
        size = shape[1]
        lat_ref[level, :, :size] = high
        lat_ref[level, :, size : 2 * size] = low
        lat_ref[level, :, 2 * size :] = high


def pack_kernel(perts_ref, even_ref, odd_ref, east_ref, west_ref, above_ref, below_ref):
    rows = east_ref.shape[1]
    turned = lax.axis_index("gy") % 2 == 1
    width = perts_ref.shape[2]
    lane = iota((rows, LANES), 1)
    east = jnp.zeros((rows, LANES), F32)
    west = jnp.zeros((rows, LANES), F32)
    for k in range(GROUP):
        t, level = k // 2, k % 2
        own = perts_ref[k]
        even, odd = even_ref[k].astype(F32), odd_ref[k].astype(F32)
        above = jnp.where(turned, even, odd)
        below = jnp.where(turned, odd, even)
        above_ref[k] = above.astype(BF16)
        below_ref[k] = below.astype(BF16)
        whole = jnp.concatenate([own.astype(F32), above, below], 0)
        last = whole[:, width - LANES :]
        first = whole[:, :LANES]
        slot = level * (LANES // 2) + t * HB
        other = (1 - level) * (LANES // 2) + t * HB
        last = pltpu.roll(last, (slot + HB) % LANES, 1)
        first = first if other == 0 else pltpu.roll(first, other, 1)
        east = jnp.where(lane >> 3 == slot // HB, last, east)
        west = jnp.where(lane >> 3 == other // HB, first, west)
    east_ref[0] = east.astype(BF16)
    west_ref[0] = west.astype(BF16)


def local_kernel(
    alpha_ref, perts_ref, lon_ref, lat_ref, token_ref, sum_ref, rows_ref, cols_ref, stack_ref
):
    height, width = alpha_ref.shape[1], alpha_ref.shape[2]

    @pl.when(pl.program_id(0) == 0)
    def _():
        sum_ref[...] = jnp.zeros_like(sum_ref)

    def put(level, start, value):
        high, low = split(value)
        stop = start + value.shape[1]
        stack_ref[level, :height, start:stop] = high
        stack_ref[level, height : 2 * height, start:stop] = high
        stack_ref[level, 2 * height :, start:stop] = low

    for level in range(2):
        packed = jnp.zeros((height, LANES), F32)
        for t in range(MEMBERS):
            field = alpha_ref[2 * t + level]
            both = dot(jnp.concatenate([field, field], 1), lon_ref[level, t])
            put(level, t * width, both[:, :width])
            packed = packed + both[:, width:]
        put(level, MEMBERS * width, packed)
    for level in range(2):
        total = sum_ref[level]
        for pair in range(MEMBERS // 2):
            base = 2 * pair * width
            wide = dot(lat_ref[level], stack_ref[level, :, base : base + 2 * width])
            for side in range(2):
                k = 2 * (2 * pair + side) + level
                field = wide[:, side * width : (side + 1) * width]
                total = total + perts_ref[k].astype(F32) * field[:height]
                rows_ref[k] = field[height:]
        sum_ref[level] = total
        cols_ref[0, level] = dot(lat_ref[level], stack_ref[level, :, MEMBERS * width :])


def stacked_cell(index, size, base):
    cell = row_of(index, size)
    low = index - base
    cell = jnp.where(index < size + 2 * HB, cell, NOWHERE)
    cell = jnp.where((low >= 0) & (low < STRIP), low - 2 * HB, cell)
    return jnp.where((low >= STRIP) & (low < 2 * STRIP), low - STRIP + size - HB, cell)


def interpolate(cell, index, weight):
    near = jnp.where(cell == index, 1.0 - weight, 0.0)
    return near + jnp.where(cell == index + 1, weight, 0.0)


def seal(axis, next_ref, previous_ref):
    place = lax.axis_index(axis)

    @pl.when(place == lax.axis_size(axis) - 1)
    def _():
        next_ref[...] = jnp.zeros_like(next_ref)

    @pl.when(place == 0)
    def _():
        previous_ref[...] = jnp.zeros_like(previous_ref)


def rows_kernel(perts_ref, even_ref, odd_ref, sems):
    height = perts_ref.shape[1]
    place = lax.axis_index("gy")

    def fill(even, odd):
        copies = [
            pltpu.make_async_copy(perts_ref.at[:, even : even + HB], even_ref, sems.at[0]),
            pltpu.make_async_copy(perts_ref.at[:, odd : odd + HB], odd_ref, sems.at[1]),
        ]
        for copy in copies:
            copy.start()
        for copy in copies:
            copy.wait()

    @pl.when(place % 2 == 0)
    def _():
        fill(height - HB, 0)

    @pl.when(place % 2 == 1)
    def _():
        fill(0, height - HB)

    @pl.when((place == 0) | (place == lax.axis_size("gy") - 1))
    def _():
        odd_ref[...] = jnp.zeros_like(odd_ref)


def table(index, weight):
    size = index.shape[-1]
    row = iota((8, size), 0)
    return jnp.where(
        row == 0, index.astype(F32).reshape(1, size), jnp.where(row == 1, weight.reshape(1, size), 0.0)
    )


def fine_cols_kernel(target_ref, weight_ref, index_ref, share_ref, east_ref, west_ref):
    cols = target_ref.shape[2]
    for a, ref in enumerate((target_ref, weight_ref)):
        for level in range(2):
            start = (2 * a + level) * SKIRT
            east_ref[start : start + SKIRT] = ref[level, :, cols - LANES :].T[LANES - SKIRT :]
            west_ref[start : start + SKIRT] = ref[level, :, :LANES].T[:SKIRT]
    lon = table(index_ref[...], share_ref[...])
    east_ref[4 * SKIRT :, :LANES] = lon[:, cols - LANES :]
    west_ref[4 * SKIRT :, :LANES] = lon[:, :LANES]


def fine_rows_kernel(
    target_ref, weight_ref, index_ref, share_ref, west_ref, east_ref, order_ref, next_ref, previous_ref,
    token_ref,
):
    rows = target_ref.shape[1]
    for a, ref in enumerate((target_ref, weight_ref)):
        for level in range(2):
            start = (2 * a + level) * SKIRT
            next_ref[start : start + SKIRT] = ref[level, rows - SKIRT :]
            previous_ref[start : start + SKIRT] = ref[level, :SKIRT]
    lat = table(index_ref[...], share_ref[...])
    for side, ref in enumerate((west_ref, east_ref)):
        lanes = slice(side * LANES, (side + 1) * LANES)
        next_ref[4 * SKIRT : 8 * SKIRT, lanes] = ref[: 4 * SKIRT, rows - LANES :]
        previous_ref[4 * SKIRT : 8 * SKIRT, lanes] = ref[: 4 * SKIRT, :LANES]
    next_ref[8 * SKIRT :, :LANES] = lat[:, rows - LANES :]
    previous_ref[8 * SKIRT :, :LANES] = lat[:, :LANES]
    token_ref[...] = lat[:, :LANES]
    seal("gy", next_ref, previous_ref)


def frame_kernel(
    sum_ref, rows_ref, cols_ref, above_ref, below_ref, west_ref, east_ref, out_ref
):
    height, width = sum_ref.shape[1], sum_ref.shape[2]
    ext = height + 2 * HB
    groups = west_ref.shape[0]
    half = iota((ext, LANES), 1) < LANES // 2
    for level in range(2):
        edge = jnp.zeros((2 * HB, width), F32)
        packed = jnp.zeros((ext, LANES), F32)
        for group in range(groups):
            for t in range(MEMBERS):
                k = group * GROUP + 2 * t + level
                halo = jnp.concatenate([above_ref[k].astype(F32), below_ref[k].astype(F32)], 0)
                edge = edge + halo * rows_ref[k]
            west = west_ref[group].astype(F32)
            east = east_ref[group].astype(F32)
            cell = jnp.where(half, west, east) if level == 0 else jnp.where(half, east, west)
            packed = packed + cell * cols_ref[group, level]
        column = packed_column(iota((LANES, LANES), 0), level, width)
        slot = iota((LANES, LANES), 1)
        target = jnp.where(slot < HB, slot - HB, jnp.where(slot < 2 * HB, slot - HB + width, NOWHERE))
        gather = (column == target).astype(BF16)
        high, low = split(packed)
        out_ref[level, :height, :width] = sum_ref[level]
        out_ref[level, height:, :width] = edge
        out_ref[level, :, width:] = dot(high, gather) + dot(low, gather)


def total_kernel(mine_ref, other_ref, total_ref, next_ref, previous_ref):
    total = mine_ref[...] + other_ref[...]
    height = total.shape[1] - 2 * HB
    total_ref[...] = total
    next_ref[:, : 2 * HB] = total[:, height - 2 * HB : height]
    next_ref[:, 2 * HB :] = total[:, height + HB :]
    previous_ref[:, :HB] = total[:, height : height + HB]
    previous_ref[:, HB:] = total[:, : 2 * HB]
    seal("gy", next_ref, previous_ref)


def strips_kernel(width, total_ref, above_ref, below_ref, stack_ref, east_ref, west_ref):
    ext, lanes = total_ref.shape[1], total_ref.shape[2]
    rows = stack_ref.shape[1]
    column = stacked_cell(iota((STRIP, lanes), 1), width, lanes)
    number = iota((STRIP, lanes), 0)
    pick_east = (column == number + width - 2 * HB).astype(BF16)
    pick_west = (column == number - HB).astype(BF16)
    for level in range(2):
        stack_ref[level, :ext] = total_ref[level]
        stack_ref[level, ext : ext + STRIP] = above_ref[level]
        stack_ref[level, ext + STRIP : ext + 2 * STRIP] = below_ref[level]
        stack_ref[level, ext + 2 * STRIP :] = jnp.zeros((rows - ext - 2 * STRIP, lanes), F32)
        high, low = split(stack_ref[level])
        part = slice(level * STRIP, (level + 1) * STRIP)
        east_ref[part] = dot(pick_east, high, (1, 1)) + dot(pick_east, low, (1, 1))
        west_ref[part] = dot(pick_west, high, (1, 1)) + dot(pick_west, low, (1, 1))


def fine_maps_kernel(
    height,
    width,
    lon_total,
    stack_ref,
    lat_index_ref,
    lat_share_ref,
    lon_index_ref,
    lon_share_ref,
    west_ref,
    east_ref,
    above_ref,
    below_ref,
    part_ref,
    beyond_ref,
    lat_map_ref,
    strip_map_ref,
    side_map_ref,
    lat_back_ref,
    back_ref,
    side_back_ref,
    side_target_ref,
    side_weight_ref,
):
    ext = height + 2 * HB
    span, cols = part_ref.shape[1], part_ref.shape[2]
    tall, lanes = stack_ref.shape[1], stack_ref.shape[2]
    lane = iota((8, LANES), 1)
    first = iota((8, LANES), 0) == 0

    def side(low, high):
        low = pltpu.roll(low, SKIRT, 1)
        high = pltpu.roll(high, SKIRT, 1)
        blank = jnp.where(first, 1.0e6, 0.0)
        return jnp.where(lane < SKIRT, low, jnp.where(lane < 2 * SKIRT, high, blank))

    def corner(low, high):
        spot = iota(low.shape, 1)
        low = pltpu.roll(low, SKIRT, 1)
        high = pltpu.roll(high, SKIRT, 1)
        return jnp.where(spot < SKIRT, low, jnp.where(spot < 2 * SKIRT, high, 0.0))

    def keep(ref, value):
        high, low = split(value)
        ref[0] = high
        ref[1] = low
        return high, low

    lat_side = side(above_ref[8 * SKIRT :, :LANES], below_ref[8 * SKIRT :, :LANES])
    lat = jnp.concatenate([table(lat_index_ref[...], lat_share_ref[...]), lat_side], 1)
    lon_side = side(west_ref[4 * SKIRT :, :LANES], east_ref[4 * SKIRT :, :LANES])
    lon = jnp.concatenate([table(lon_index_ref[...], lon_share_ref[...]), lon_side], 1)
    lat_cell = lat[0:1].astype(jnp.int32) - lax.axis_index("gy") * height
    lat_share = lat[1:2]
    lon_cell = lon[0:1].astype(jnp.int32) - lax.axis_index("gx") * width
    lon_cell = jnp.where(lon_cell < -(lon_total // 2), lon_cell + lon_total, lon_cell)
    wrap = (lon_cell >= lon_total // 2) & (lon_cell < lon_total)
    lon_cell = jnp.where(wrap, lon_cell - lon_total, lon_cell)
    lon_share = lon[1:2]
    upright = jnp.concatenate([lat_cell.astype(F32), lat_share, jnp.zeros((6, span), F32)], 0).T
    lat_cell_up, lat_share_up = upright[:, 0:1].astype(jnp.int32), upright[:, 1:2]
    upright = jnp.concatenate(
        [lon_cell.astype(F32), lon_share, jnp.zeros((6, cols + LANES), F32)], 0
    ).T
    lon_cell_up, lon_share_up = upright[:, 0:1].astype(jnp.int32), upright[:, 1:2]
    beside = slice(cols, cols + 2 * SKIRT)

    lat_map = keep(
        lat_map_ref,
        interpolate(stacked_cell(iota((span, tall), 1), height, ext), lat_cell_up, lat_share_up),
    )
    broad = lanes + LANES
    lon_map = interpolate(
        stacked_cell(iota((broad, cols), 0), width, lanes), lon_cell[:, :cols], lon_share[:, :cols]
    )
    keep(strip_map_ref, lon_map[lanes:])
    lon_map = split(lon_map[:lanes])
    side_map = interpolate(
        stacked_cell(iota((2 * SKIRT, broad), 1), width, lanes),
        lon_cell_up[beside],
        lon_share_up[beside],
    )
    keep(side_map_ref, side_map[:, lanes:])
    side_map = split(side_map[:, :lanes])
    keep(lat_back_ref, interpolate(row_of(iota((ext, span), 0), height), lat_cell, lat_share))
    for level in range(2):
        wide = split(dot3(lat_map, stack_ref[level]))
        part_ref[level] = dot3(wide, lon_map)
        beyond_ref[level] = dot3(side_map, wide, (1, 1))
        lane_wide = iota((1, width + LANES), 1)
        column = jnp.where(
            lane_wide < width, lane_wide, packed_column(lane_wide - width, level, width)
        )
        keep(back_ref.at[level], interpolate(column, lon_cell_up[:cols], lon_share_up[:cols]))
        keep(side_back_ref.at[level], interpolate(column, lon_cell_up[beside], lon_share_up[beside]))
        for array, out_ref in enumerate((side_target_ref, side_weight_ref)):
            start = (2 * array + level) * SKIRT
            for number, ref in enumerate((west_ref, east_ref)):
                tile = slice(number * LANES, (number + 1) * LANES)
                rows = slice(4 * SKIRT + start, 5 * SKIRT + start)
                at = slice(number * SKIRT, (number + 1) * SKIRT)
                out_ref[level, at, : span - LANES] = ref[start : start + SKIRT]
                out_ref[level, at, span - LANES :] = corner(above_ref[rows, tile], below_ref[rows, tile])


def fine_kernel(
    strip_west_ref,
    strip_east_ref,
    target_ref,
    weight_ref,
    above_ref,
    below_ref,
    part_ref,
    beyond_ref,
    lat_map_ref,
    strip_map_ref,
    side_map_ref,
    lat_back_ref,
    back_ref,
    side_back_ref,
    side_target_ref,
    side_weight_ref,
    inc_ref,
    own_ref,
    edge_ref,
    wide_ref,
    miss_ref,
    by_lon_ref,
):
    width = own_ref.shape[2]
    rows = target_ref.shape[1]
    span = part_ref.shape[1]
    wide_ref[...] = jnp.zeros_like(wide_ref)

    def kept(ref):
        return ref[0], ref[1]

    used = rows + 2 * SKIRT
    for level in range(2):
        part = slice(level * STRIP, (level + 1) * STRIP)
        strips = jnp.concatenate([strip_west_ref[part], strip_east_ref[part]], 0)
        wide_ref[level, :, : 2 * STRIP] = dot3(kept(lat_map_ref), strips, (1, 1))
    for level in range(2):
        wide = split(wide_ref[level, :used])
        increment = part_ref[level, :used] + dot3(wide, kept(strip_map_ref))
        inc_ref[level] = increment[:rows]
        miss_ref[level, :rows] = weight_ref[level] * (increment[:rows] - target_ref[level])
        target_rows = slice(level * SKIRT, (level + 1) * SKIRT)
        weight_rows = slice((2 + level) * SKIRT, (3 + level) * SKIRT)
        for number, ref in enumerate((above_ref, below_ref)):
            start = rows + number * SKIRT
            difference = increment[start : start + SKIRT] - ref[target_rows]
            miss_ref[level, start : start + SKIRT] = ref[weight_rows] * difference
    for level in range(2):
        wide = split(wide_ref[level])
        beyond = beyond_ref[level] + dot3(kept(side_map_ref), wide, (1, 1))
        beyond = side_weight_ref[level] * (beyond - side_target_ref[level])
        back_ref_level = kept(back_ref.at[level])
        by_lon_ref[level, :used] = dot3(miss_ref[level, :used], back_ref_level)
        by_lon_ref[level, used:] = jnp.zeros((span - used, width + LANES), F32)
        by_lon_ref[level] += dot3(beyond, kept(side_back_ref.at[level]), (0, 0))
    for level in range(2):
        residual = dot3(kept(lat_back_ref), by_lon_ref[level])
        own_ref[level] = residual[:, :width]
        edge_ref[level] = residual[:, width:]


def gradient_kernel(
    alpha_ref, perts_ref, above_ref, below_ref, west_ref, east_ref, own_ref, edge_ref, lon_ref, lat_ref,
    out_ref, stack_ref,
):
    height, width = alpha_ref.shape[1], alpha_ref.shape[2]
    ext = height + 2 * HB

    half = iota((ext, LANES), 1) < LANES // 2

    def stacked(value):
        high, low = split(value)
        return jnp.concatenate([high, high, low], 0)

    for level in range(2):
        west = west_ref[0].astype(F32)
        east = east_ref[0].astype(F32)
        cell = jnp.where(half, west, east) if level == 0 else jnp.where(half, east, west)
        side = dot(lat_ref[level], stacked(cell * edge_ref[level]))
        side = jnp.concatenate(split(side), 0)
        for p in range(MEMBERS // 2):
            columns = []
            for t in (2 * p, 2 * p + 1):
                k = 2 * t + level
                field = jnp.concatenate(
                    [perts_ref[k].astype(F32), above_ref[k].astype(F32), below_ref[k].astype(F32)], 0
                )
                columns.append(stacked(field * own_ref[level]))
            both = dot(lat_ref[level], jnp.concatenate(columns, 1))
            for number in range(2):
                k = 2 * (2 * p + number) + level
                high, low = split(both[:, number * width : (number + 1) * width])
                stack_ref[k, :height, :width] = high
                stack_ref[k, height:, :width] = low
                stack_ref[k, :, width:] = side
    for level in range(2):
        for t in range(MEMBERS):
            k = 2 * t + level
            both = dot(stack_ref[k], lon_ref[level, t])
            total = both[:height, :width] + both[:height, width:] + both[height:, :width]
            out_ref[k] = alpha_ref[k].astype(F32) + total


def exchange(to_next, to_previous, axis):
    count = lax.axis_size(axis)
    forward = [(i, (i + 1) % count) for i in range(count)]
    backward = [(target, source) for source, target in forward]
    ahead = lax.ppermute(to_next, axis, forward)
    behind = lax.ppermute(to_previous, axis, backward)
    return ahead, behind


def exchange_pairs(to_even, to_odd, axis):
    count = lax.axis_size(axis)
    even = [(i, i ^ 1) for i in range(count)]
    odd = [(i, min(max(i + 1 if i % 2 else i - 1, 0), count - 1)) for i in range(count)]
    ahead = lax.ppermute(to_even, axis, even)
    behind = lax.ppermute(to_odd, axis, odd)
    return ahead, behind


def vmem(*shape):
    return pl.BlockSpec(shape, lambda s: (0,) * len(shape))


def grouped(*shape):
    return pl.BlockSpec(shape, lambda s: (s,) + (0,) * (len(shape) - 1))


def shaped(shape, dtype=F32):
    return jax.ShapeDtypeStruct(shape, dtype)


def whole_step(
    alpha_fields,
    member_perts,
    band_widths,
    lat_index,
    lat_weight,
    lon_index,
    lon_weight,
    innovation,
    obs_weight,
):
    members, levels, height, width = alpha_fields.shape
    fields = members * levels
    groups = fields // GROUP
    ext = height + 2 * HB
    fine_h, fine_w = innovation.shape[1], innovation.shape[2]
    alpha = alpha_fields.reshape(fields, height, width)
    perts = member_perts.reshape(fields, height, width)
    smem = pl.BlockSpec(memory_space=pltpu.SMEM)
    anywhere = pl.BlockSpec(memory_space=pl.ANY)
    whole = pl.BlockSpec(memory_space=pltpu.VMEM)
    scale = width // LANES
    lanes = rounded(width + 2 * HB, LANES)
    tall = rounded(ext + 2 * STRIP, LANES)

    def call(kernel, out_shape, flops=10**8, grant=4, **more):
        semantics = ("arbitrary",) if "grid" in more else ()
        return pl.pallas_call(
            kernel,
            out_shape=out_shape,
            compiler_params=pltpu.CompilerParams(
                dimension_semantics=semantics, vmem_limit_bytes=min(60, grant * scale) * 1024 * 1024
            ),
            cost_estimate=pl.CostEstimate(flops=flops, bytes_accessed=10**6, transcendentals=0),
            **more,
        )

    edge = shaped((fields, HB, width), BF16)
    to_even, to_odd = call(
        rows_kernel,
        [edge, edge],
        in_specs=[pl.BlockSpec(memory_space=pltpu.HBM)],
        out_specs=[pl.BlockSpec(memory_space=pltpu.VMEM)] * 2,
        scratch_shapes=[pltpu.SemaphoreType.DMA((2,))],
    )(perts)
    even, odd = exchange_pairs(to_even, to_odd, "gy")
    lon_shape, lat_shape = (2, MEMBERS, 2 * width, width + LANES), (2, ext, 3 * height)
    lon_back_shape, lat_back_shape = (2, MEMBERS, width + LANES, 2 * width), (2, height, 3 * ext)
    lon_table, lat_table = call(
        functools.partial(tables_kernel, False),
        [shaped(lon_shape, BF16), shaped(lat_shape, BF16)],
        grant=8,
        in_specs=[smem],
    )(band_widths)

    side = shaped((4 * SKIRT + 8, fine_h))
    to_next, to_previous = call(fine_cols_kernel, [side, side])(
        innovation, obs_weight, lon_index, lon_weight
    )
    fine_west, fine_east = exchange(to_next, to_previous, "gx")

    packed = shaped((groups, ext, LANES), BF16)
    to_next, to_previous, above, below = call(
        pack_kernel,
        [packed, packed, edge, edge],
        grant=8,
        grid=(groups,),
        in_specs=[grouped(GROUP, height, width)] + [grouped(GROUP, HB, width)] * 2,
        out_specs=[grouped(1, ext, LANES)] * 2 + [grouped(GROUP, HB, width)] * 2,
    )(perts, even, odd)
    west, east = exchange(to_next, to_previous, "gx")

    strip = shaped((8 * SKIRT + 8, fine_w))
    to_next, to_previous, token = call(
        fine_rows_kernel, [strip, strip, shaped((8, LANES))], in_specs=[whole] * 6 + [anywhere]
    )(innovation, obs_weight, lat_index, lat_weight, fine_west, fine_east, to_next)
    fine_above, fine_below = exchange(to_next, to_previous, "gy")

    partial, edge_rows, edge_cols = call(
        local_kernel,
        [
            shaped((2, height, width)),
            shaped((fields, 2 * HB, width)),
            shaped((groups, 2, ext, LANES)),
        ],
        flops=10**10,
        grant=16,
        grid=(groups,),
        in_specs=[
            grouped(GROUP, height, width),
            grouped(GROUP, height, width),
            whole,
            whole,
            anywhere,
        ],
        out_specs=[
            vmem(2, height, width),
            grouped(GROUP, 2 * HB, width),
            grouped(1, 2, ext, LANES),
        ],
        scratch_shapes=[
            pltpu.VMEM((2, 3 * height, MEMBERS * width + LANES), BF16),
        ],
    )(alpha, perts, lon_table, lat_table, token)

    framed = call(
        frame_kernel, shaped((2, ext, width + LANES)), in_specs=[whole] * 7
    )(partial, edge_rows, edge_cols, above, below, west, east)
    count = lax.axis_size("ma")
    other = lax.ppermute(framed, "ma", [(i, (i + 1) % count) for i in range(count)])
    strip = shaped((2, STRIP, lanes))
    framed, to_next, to_previous = call(
        total_kernel, [shaped((2, ext, lanes)), strip, strip]
    )(framed, other)
    lon_back, lat_back = call(
        functools.partial(tables_kernel, True),
        [shaped(lon_back_shape, BF16), shaped(lat_back_shape, BF16)],
        grant=8,
        in_specs=[smem],
    )(band_widths)
    north, south = exchange(to_next, to_previous, "gy")
    strip = shaped((2 * STRIP, tall))
    stack, to_next, to_previous = call(
        functools.partial(strips_kernel, width), [shaped((2, tall, lanes)), strip, strip]
    )(framed, north, south)
    strip_west, strip_east = exchange(to_next, to_previous, "gx")

    lon_total = width * lax.axis_size("gx")
    span = fine_h + LANES
    pair = (2, 2 * SKIRT, span)
    maps = call(
        functools.partial(fine_maps_kernel, height, width, lon_total),
        [
            shaped((2, span, fine_w)),
            shaped(pair),
            shaped((2, span, tall), BF16),
            shaped((2, LANES, fine_w), BF16),
            shaped((2, 2 * SKIRT, LANES), BF16),
            shaped((2, ext, span), BF16),
            shaped((2, 2, fine_w, width + LANES), BF16),
            shaped((2, 2, 2 * SKIRT, width + LANES), BF16),
            shaped(pair),
            shaped(pair),
        ],
        grant=16,
        in_specs=[whole] * 9,
    )(
        stack,
        lat_index,
        lat_weight,
        lon_index,
        lon_weight,
        fine_west,
        fine_east,
        fine_above,
        fine_below,
    )
    increment, own, edge = call(
        fine_kernel,
        [shaped((2, fine_h, fine_w)), shaped((2, ext, width)), shaped((2, ext, LANES))],
        grant=16,
        in_specs=[whole] * 16,
        scratch_shapes=[
            pltpu.VMEM((2, span, LANES), F32),
            pltpu.VMEM((2, span, fine_w), F32),
            pltpu.VMEM((2, span, width + LANES), F32),
        ],
    )(strip_west, strip_east, innovation, obs_weight, fine_above, fine_below, *maps)

    gradient = call(
        gradient_kernel,
        shaped((fields, height, width)),
        grant=16,
        grid=(groups,),
        in_specs=[
            grouped(GROUP, height, width),
            grouped(GROUP, height, width),
            grouped(GROUP, HB, width),
            grouped(GROUP, HB, width),
            grouped(1, ext, LANES),
            grouped(1, ext, LANES),
            vmem(2, ext, width),
            vmem(2, ext, LANES),
            whole,
            whole,
        ],
        out_specs=grouped(GROUP, height, width),
        scratch_shapes=[pltpu.VMEM((GROUP, 2 * height, width + LANES), BF16)],
    )(alpha, perts, above, below, west, east, own, edge, lon_back, lat_back)
    return increment, gradient.reshape(alpha_fields.shape)


def solution(mesh):
    placed = (
        P("ma", None, "gy", "gx"),
        P("ma", None, "gy", "gx"),
        P(),
        P("gy"),
        P("gy"),
        P("gx"),
        P("gx"),
        P(None, "gy", "gx"),
        P(None, "gy", "gx"),
    )
    return jax.shard_map(
        whole_step,
        mesh=mesh,
        in_specs=placed,
        out_specs=(P(None, "gy", "gx"), P("ma", None, "gy", "gx")),
        check_vma=False,
    )
```
